128 devices in a mesh: sp: 8 (over x, y_lo), ep: 16 (over z, y_hi, core).
Axes of the slice: x: 4, y: 4 (y_hi: 2, y_lo: 2; y = y_hi * 2 + y_lo), z: 4, core: 2. Of those that a mesh axis runs over, the one named last changes fastest.
Arguments:
- residual: bfloat16 [16384, 4096], P(('sp', 'ep')), may hold values from -40 to 40
- queries: bfloat16 [16384, 4096], P(('sp', 'ep')), may hold values from -6 to 6
- key_rows: bfloat16 [16384, 1024], P(('sp', 'ep')), may hold values from -6 to 6
- value_rows: bfloat16 [16384, 1024], P(('sp', 'ep')), may hold values from -6 to 6
- visible: int32 [128, 9], replicated, may hold values from 0 to 1, as said below
- out_proj: bfloat16 [4096, 4096], P(('sp', 'ep')), may hold values from -0.09375 to 0.09375
- norm_gain: float32 [4096], replicated, may hold values from 0.5 to 1.5
- expert_ids: int32 [16384, 2], P(('sp', 'ep')), may hold values from 0 to 7, all different within a row; in each aligned block of 128 rows (0 to 127, 128 to 255, ...) at most 40 rows name the same one
- route_weight: float32 [16384, 2], P(('sp', 'ep')), may hold values from 0.2 to 1
- expert_gate: bfloat16 [2, 7168, 4096], P(None, 'ep'), may hold values from -0.09375 to 0.09375
- expert_up: bfloat16 [2, 7168, 4096], P(None, 'ep'), may hold values from -0.09375 to 0.09375
- expert_down: bfloat16 [2, 7168, 4096], P(None, 'ep'), may hold values from -0.0625 to 0.0625
Outputs:
- layer_out: bfloat16 [16384, 4096], P(('sp', 'ep'))
The draws below stay inside these ranges and needn't reach their ends.
Inputs may be any that keep to these rules, and one draw needn't show every extreme that they name: The sequence is packed with documents that are runs of whole blocks of 128 tokens, the first of them 9 blocks or longer; visible[q, d] is 1 exactly when block q - d exists and lies in the document of block q, so visible[q, 0] = 1. `expert_ids`: each token names two different experts. Among the 128 tokens of one block no expert is named by more than 40 tokens.
All inputs are finite; a program needn't handle non-finite values.
Results may differ from the reference program's by a relative error of at most 0.0065.
Values may be sent and summed in bfloat16 or wider, within the bound.
No kernel may reach another device: no remote copies, remote signals or barrier semaphores. Data moves between devices by JAX's collectives and lax.ppermute only.
A program may use at most 128 MiB of HBM per device.

```python
import math
import jax
import jax.numpy as jnp
import numpy as np
from jax import lax

D = 4096
HEADS = 32
KV_HEADS = 8
HEAD = 128
EXPERTS = 8
EXP_WIN = 2
FF_WIN = 7168
TOK_DEV = 128
TOKENS = 16384
BLOCKS = 128
SPAN = 9
CAP = 40
N_SP = 8
N_EP = 16


def paired_fields(key):
    key_query, key_keys = jax.random.split(key, 2)
    query_field = jnp.clip(jax.random.normal(key_query, (TOKENS, HEADS * HEAD), jnp.float32), -6.0, 6.0)
    key_field = jnp.clip(jax.random.normal(key_keys, (TOKENS, KV_HEADS * HEAD), jnp.float32), -6.0, 6.0)
    return (query_field, key_field)


def draw_queries(key, part):
    query_field, key_field = paired_fields(jax.random.fold_in(key, 71))
    return query_field.astype(jnp.bfloat16)


def draw_key_rows(key, part):
    query_field, key_field = paired_fields(jax.random.fold_in(key, 71))
    return key_field.astype(jnp.bfloat16)


def draw_residual(key, part):
    key_base = jax.random.fold_in(jax.random.fold_in(key, 13), 0)
    base_field = jnp.clip(jax.random.normal(key_base, (TOKENS, D), jnp.float32), -4.0, 4.0)
    return base_field.astype(jnp.bfloat16)


def draw_visible(key, part):
    doc_starts = jax.random.randint(jax.random.fold_in(key, 29), (BLOCKS,), 0, 5) == 0
    block_number = jnp.arange(BLOCKS, dtype=jnp.int32)
    doc_starts = jnp.where(block_number < SPAN, block_number == 0, doc_starts)
    doc_index = jnp.cumsum(doc_starts.astype(jnp.int32))
    query_block = block_number[:, None]
    key_block = query_block - jnp.arange(SPAN, dtype=jnp.int32)[None, :]
    same_doc = doc_index[query_block] == doc_index[jnp.clip(key_block, 0, BLOCKS - 1)]
    return ((key_block >= 0) & same_doc).astype(jnp.int32)


def shard_levels(own_key, extent, pieces, least, top_value):
    gain, own = 1.0, jax.random.fold_in(own_key, 6)
    for dim, blocks in pieces:
        draws = jnp.exp(jax.random.uniform(jax.random.fold_in(own, dim), (blocks,), jnp.float32, least / len(pieces), top_value / len(pieces)))
        gain = gain * jnp.repeat(draws, extent[dim] // blocks).reshape([-1 if axis == dim else 1 for axis in range(len(extent))])
    return gain


def routed_block(stream_key, own, number, rows, amount, top, limit, lean):
    sequence = jax.random.permutation(stream_key, amount)
    heavy_load, common = shares(amount, rows * top, limit, lean, True), shares(amount, rows * top, limit, lean, False)
    places = jnp.arange(amount)

    def named(sizes, turn):
        used = int((sizes > 0).sum())
        fixed = max(1, used // 4)
        moved = fixed + (places - fixed + turn * (used - fixed)) % max(1, amount - fixed)
        return jnp.zeros((amount,), jnp.int32).at[sequence[jnp.where(places < fixed, places, moved)]].set(jnp.asarray(sizes, jnp.int32))

    sizes = jnp.where(number % 4 == 0, named(heavy_load, number // 4), named(common, number - number // 4 - 1))
    mixed = jax.random.permutation(jax.random.fold_in(own, 3), amount)
    giver, sink = mixed[0:amount // 2 * 2:2], mixed[1:amount // 2 * 2:2]
    room = jnp.minimum(sizes[giver] - 1, limit - sizes[sink]) // 2
    room = jnp.where((giver == sequence[0]) | (sink == sequence[0]) | (sizes[sink] == 0), 0, jnp.maximum(room, 0))
    moved = jax.random.randint(jax.random.fold_in(own, 4), (amount // 2,), 0, 1 << 20) % (room + 1)
    sizes = sizes.at[giver].add(-moved).at[sink].add(moved)
    items = jnp.searchsorted(jnp.cumsum(sizes), jnp.arange(rows * top), side="right").astype(jnp.int32)
    listing = items.reshape(top, rows).T
    listing = listing[jax.random.permutation(jax.random.fold_in(own, 1), rows)]
    turn = jax.random.randint(jax.random.fold_in(own, 2), (rows, 1), 0, top)
    return jnp.take_along_axis(listing, (jnp.arange(top)[None, :] + turn) % top, axis=1)


def shares(count, total, limit, lean, full):
    loads = [(1 << 20) // math.isqrt(rank ** lean) + 1 for rank in range(1, count + 1)]
    largest = limit if full else min(limit, max(-(-total // count), total * loads[0] // sum(loads)))
    least = 1 if total - largest >= count - 1 else 0
    given, surplus = [largest] + [least] * (count - 1), total - largest - least * (count - 1)
    while surplus > 0:
        free = [i for i in range(1, count) if given[i] < largest] or [i for i in range(1, count) if given[i] < limit]
        pool, left = sum([loads[i] for i in free]), surplus
        for i in free:
            more = min(limit - given[i], max(1, left * loads[i] // pool), surplus)
            given[i] = given[i] + more
            surplus = surplus - more
    return np.array(given)


def noise(own_key, shape, spread, bound, pieces=(), held_as=jnp.bfloat16):
    entries = jax.random.normal(own_key, shape, jnp.float32) * spread
    if len(pieces) > 0:
        entries = shard_levels(own_key, shape, pieces, -0.22, 0.18) * entries
    return jnp.clip(entries, min=-bound, max=bound).astype(held_as)


def setup_inputs(seed: int = 0) -> dict:
    arg_keys = jax.random.split(jax.random.key(seed), 13)
    residual = draw_residual(jax.random.fold_in(arg_keys[12], 71), 0)
    queries = draw_queries(jax.random.fold_in(arg_keys[12], 71), 0)
    key_rows = draw_key_rows(jax.random.fold_in(arg_keys[12], 71), 0)
    value_rows = noise(arg_keys[3], (TOKENS, KV_HEADS * HEAD), 1.0, 6.0, ((0, 128),))
    visible = draw_visible(jax.random.fold_in(arg_keys[12], 71), 0)
    out_proj = noise(arg_keys[5], (HEADS * HEAD, D), (HEADS * HEAD) ** -0.5, 0.09375, ((0, 128),))
    norm_gain = jnp.clip(1.0 + 0.1 * jax.random.normal(arg_keys[6], (D,), jnp.float32), 0.5, 1.5)
    expert_ids_keys = jax.random.split(jax.random.fold_in(arg_keys[7], 1), TOKENS // TOK_DEV)
    expert_ids_turns = jax.random.permutation(jax.random.fold_in(arg_keys[7], 3), TOKENS // TOK_DEV)
    expert_ids = jax.vmap(lambda own, number: routed_block(jax.random.fold_in(arg_keys[7], 2), own, number, TOK_DEV, EXPERTS, 2, CAP, 2))(expert_ids_keys, expert_ids_turns).reshape((TOKENS, 2))
    route_weight = jnp.clip(0.2 + 0.8 * jax.random.uniform(arg_keys[8], (TOKENS, 2), jnp.float32) ** shard_levels(arg_keys[8], (TOKENS, 2), ((0, 128),), -0.2, 0.2), 0.2, 1.0)
    expert_gate = noise(arg_keys[9], (EXP_WIN, FF_WIN, D), D ** -0.5, 0.09375, ((1, 16),))
    expert_up = noise(arg_keys[10], (EXP_WIN, FF_WIN, D), D ** -0.5, 0.09375, ((1, 16),))
    expert_down = noise(arg_keys[11], (EXP_WIN, FF_WIN, D), FF_WIN ** -0.5, 0.0625, ((1, 16),))
    return dict(residual=residual, queries=queries, key_rows=key_rows, value_rows=value_rows, visible=visible, out_proj=out_proj, norm_gain=norm_gain, expert_ids=expert_ids, route_weight=route_weight, expert_gate=expert_gate, expert_up=expert_up, expert_down=expert_down)


def attend_block(block_index, queries, key_padded, value_padded, visible):
    grouping = HEADS // KV_HEADS
    start_row = (block_index * TOK_DEV).astype(jnp.int32)
    query_block = lax.dynamic_slice_in_dim(queries, start_row, TOK_DEV, 0).astype(jnp.float32)
    query_block = query_block.reshape(TOK_DEV, KV_HEADS, grouping, HEAD)
    key_block = lax.dynamic_slice_in_dim(key_padded, start_row, SPAN * TOK_DEV, 0)
    key_block = key_block.reshape(SPAN, TOK_DEV, KV_HEADS, HEAD)[::-1]
    value_block = lax.dynamic_slice_in_dim(value_padded, start_row, SPAN * TOK_DEV, 0)
    value_block = value_block.reshape(SPAN, TOK_DEV, KV_HEADS, HEAD)[::-1]
    scores = jnp.einsum('tgrh,dugh->grtdu', query_block, key_block) * (1.0 / math.sqrt(HEAD))
    seen = lax.dynamic_index_in_dim(visible, block_index, 0, keepdims=False)
    position = jnp.arange(TOK_DEV)
    distances = jnp.arange(SPAN)
    allowed = (seen[None, :, None] > 0) & ((distances[None, :, None] > 0) | (position[None, None, :] <= position[:, None, None]))
    scores = jnp.where(allowed, scores, -1e+30)
    peak = lax.optimization_barrier(jnp.max(scores, axis=(3, 4), keepdims=True))
    weights_f = jnp.where(allowed, jnp.exp(scores - peak), 0.0)
    totals = lax.optimization_barrier(jnp.sum(weights_f, axis=(3, 4)))
    weights_b = lax.optimization_barrier(weights_f.astype(jnp.bfloat16)).astype(jnp.float32)
    summed = jnp.einsum('grtdu,dugh->tgrh', weights_b, value_block)
    summed = summed / jnp.transpose(totals, (2, 0, 1))[..., None]
    return summed.astype(jnp.bfloat16).reshape(TOK_DEV, HEADS * HEAD)

def expert_block(normed_rows, chosen_ids, chosen_weight, expert_gate, expert_up, down_table):
    slice_width = FF_WIN // N_EP
    mixture = jnp.zeros((TOK_DEV, D), jnp.float32)
    for window_index in range(EXP_WIN):
        choose = chosen_ids == window_index
        member = jnp.any(choose, axis=1)
        token_weight = lax.optimization_barrier(jnp.sum(jnp.where(choose, chosen_weight, 0.0), axis=1))
        ranked = jnp.cumsum(member.astype(jnp.int32)) - member.astype(jnp.int32)
        slot_hit = (ranked[None, :] == jnp.arange(CAP, dtype=jnp.int32)[:, None]) & member[None, :]
        picked = jnp.dot(slot_hit.astype(jnp.bfloat16), normed_rows, preferred_element_type=jnp.float32).astype(jnp.bfloat16)
        gate_act = jnp.dot(picked, expert_gate[window_index].T, preferred_element_type=jnp.float32)
        up_act = jnp.dot(picked, expert_up[window_index].T, preferred_element_type=jnp.float32)
        activated = (jax.nn.silu(gate_act) * up_act).astype(jnp.bfloat16)
        slices = jnp.einsum('cje,jed->cjd', activated.astype(jnp.float32).reshape(CAP, N_EP, slice_width), down_table[window_index])
        slot_out = lax.optimization_barrier(jnp.sum(lax.optimization_barrier(slices.astype(jnp.bfloat16)).astype(jnp.float32), axis=1))
        combine = jnp.where(slot_hit, token_weight[None, :], 0.0)
        mixture = mixture + jnp.dot(combine.T, slot_out, precision=lax.Precision.HIGHEST)
    return mixture

def reference(residual, queries, key_rows, value_rows, visible, out_proj, norm_gain, expert_ids, route_weight, expert_gate, expert_up, expert_down):
    padding = (SPAN - 1) * TOK_DEV
    key_padded = jnp.pad(key_rows.astype(jnp.float32), ((padding, 0), (0, 0)))
    value_padded = jnp.pad(value_rows.astype(jnp.float32), ((padding, 0), (0, 0)))

    def one_block(block_index):
        return attend_block(block_index, queries, key_padded, value_padded, visible)
    attended = lax.map(one_block, jnp.arange(BLOCKS, dtype=jnp.int32)).reshape(TOKENS, HEADS * HEAD)
    group_width = HEADS * HEAD // N_SP
    projected = jnp.zeros((TOKENS, D), jnp.float32)
    for group_index in range(N_SP):
        lower = group_index * group_width
        upper = lower + group_width
        part = jnp.dot(attended[:, lower:upper], out_proj[lower:upper], preferred_element_type=jnp.float32)
        projected = projected + lax.optimization_barrier(part.astype(jnp.bfloat16)).astype(jnp.float32)
    hidden_sum = residual.astype(jnp.float32) + projected
    mean_square = lax.optimization_barrier(jnp.mean(hidden_sum * hidden_sum, axis=-1, keepdims=True))
    normed = (hidden_sum * lax.rsqrt(mean_square + 1e-05) * norm_gain).astype(jnp.bfloat16)
    down_table = expert_down.astype(jnp.float32).reshape(EXP_WIN, N_EP, FF_WIN // N_EP, D)

    def moe_block(packed):
        normed_rows, chosen_ids, chosen_weight = packed
        return expert_block(normed_rows, chosen_ids, chosen_weight, expert_gate, expert_up, down_table)
    expert_mix = lax.map(moe_block, (normed.reshape(BLOCKS, TOK_DEV, D), expert_ids.reshape(BLOCKS, TOK_DEV, 2), route_weight.reshape(BLOCKS, TOK_DEV, 2)))
    expert_mix = expert_mix.reshape(TOKENS, D)
    return (hidden_sum + expert_mix).astype(jnp.bfloat16)
```

```python
import math

import jax
import jax.numpy as jnp
from jax import lax
from jax.experimental import pallas as pl
from jax.experimental.pallas import tpu as pltpu
from jax.sharding import Mesh
from jax.sharding import PartitionSpec as P

HEAD = 128
CAP = 40
SIZES = (4, 2, 4, 2, 2)
AXES = ("x", "yl", "z", "h", "c")
EP = ("z", "h", "c")


def flat(coords):
    place = 0
    for size, coord in zip(SIZES, coords):
        place = place * size + coord
    return place


def moved(value, x=0, y=0, z=0, core=False):
    pairs = []
    for source in range(math.prod(SIZES)):
        rest, coords = source, []
        for size in reversed(SIZES):
            coords.append(rest % size)
            rest //= size
        cx, cyl, cz, ch, cc = reversed(coords)
        cy = (2 * ch + cyl + y) % 4
        target = ((cx + x) % 4, cy % 2, (cz + z) % 4, cy // 2, 1 - cc if core else cc)
        pairs.append((source, flat(target)))
    return lax.ppermute(value, AXES, pairs)


def later(value, blocks):
    count = math.prod(SIZES)
    return lax.ppermute(value, AXES, [(s, s + blocks) for s in range(count - blocks)])


def half_of(value, which):
    width = value.shape[-1] // 2
    return lax.dynamic_slice_in_dim(value, which * width, width, value.ndim - 1)


def by_core(first, own, other, axis):
    return jnp.where(
        first,
        jnp.concatenate([own, other], axis=axis),
        jnp.concatenate([other, own], axis=axis),
    )


def attend_kernel(seen_ref, query_ref, *refs):
    key_refs, value_refs, out_ref = refs[:5], refs[5:10], refs[10]
    keys = jnp.concatenate([ref[...] for ref in key_refs], axis=0)
    values = jnp.concatenate([ref[...] for ref in value_refs], axis=0)
    factor = math.log2(math.e) / math.sqrt(HEAD)
    tokens = 128
    row = lax.broadcasted_iota(jnp.int32, (tokens, tokens), 0)
    col = lax.broadcasted_iota(jnp.int32, (tokens, tokens), 1)
    causal = jnp.where(col <= row, 0.0, -1e30)
    for block in range(2):
        key_window = keys[block * tokens : (block + 9) * tokens]
        value_window = values[block * tokens : (block + 9) * tokens]
        hidden = [
            jnp.full((tokens, tokens), jnp.where(seen_ref[block, 8 - place] > 0, 0.0, -1e30))
            for place in range(8)
        ]
        bias = jnp.concatenate(hidden + [causal], axis=1)
        heads = []
        for head in range(4):
            query = query_ref[block * tokens : (block + 1) * tokens, head * HEAD : (head + 1) * HEAD]
            score = lax.dot_general(
                query, key_window, (((1,), (1,)), ((), ())), preferred_element_type=jnp.float32
            )
            score = score + bias
            peak = jnp.max(score, axis=1, keepdims=True)
            weight = jnp.exp2((score - peak) * factor)
            total = jnp.sum(weight, axis=1, keepdims=True)
            mixed = jnp.dot(
                weight.astype(jnp.bfloat16), value_window, preferred_element_type=jnp.float32
            )
            heads.append(mixed / total)
        for part in range(2):
            lanes = slice(part * 64, part * 64 + 64)
            joined = jnp.concatenate([head[:, lanes] for head in heads], axis=1)
            out_ref[part, 0, block * tokens : (block + 1) * tokens, :] = joined.astype(jnp.bfloat16)


def attend(seen, query, windows):
    key_specs = [pl.BlockSpec((256, HEAD), lambda j: (0, j)) for _ in windows]
    value_specs = [pl.BlockSpec((256, HEAD), lambda j: (0, 4 + j)) for _ in windows]
    return pl.pallas_call(
        attend_kernel,
        grid=(4,),
        in_specs=[
            pl.BlockSpec(memory_space=pltpu.SMEM),
            pl.BlockSpec((256, 4 * HEAD), lambda j: (0, j)),
            *key_specs,
            *value_specs,
        ],
        out_specs=pl.BlockSpec((2, 1, 256, 256), lambda j: (0, j % 2, 0, j // 2)),
        out_shape=jax.ShapeDtypeStruct((2, 2, 256, 512), jnp.bfloat16),
        name="attend",
        cost_estimate=pl.CostEstimate(
            flops=6_000_000_000, transcendentals=5_000_000, bytes_accessed=6_000_000
        ),
    )(seen, query, *windows, *windows)


def in_order(pieces, own_index):
    count = len(pieces)
    table = jnp.zeros((count, *pieces[0].shape), pieces[0].dtype)
    for step, piece in enumerate(pieces):
        table = lax.dynamic_update_index_in_dim(table, piece, (own_index - step) % count, 0)
    return table.reshape(-1, *pieces[0].shape[1:])


def local(
    residual,
    queries,
    key_rows,
    value_rows,
    visible,
    out_proj,
    norm_gain,
    expert_ids,
    route_weight,
    expert_gate,
    expert_up,
    expert_down,
):
    core = lax.axis_index("c")
    first = core == 0
    tokens, width = residual.shape
    place_y = 2 * lax.axis_index("h") + lax.axis_index("yl")

    kv_own = jnp.concatenate([half_of(key_rows, core), half_of(value_rows, core)], axis=1)
    kv_give = jnp.concatenate([half_of(key_rows, 1 - core), half_of(value_rows, 1 - core)], axis=1)
    kv_two = by_core(first, kv_own, moved(kv_give, core=True), 0)
    query_two = by_core(
        first, half_of(queries, core), moved(half_of(queries, 1 - core), core=True), 0
    )
    windows = [later(kv_two, blocks) for blocks in (8, 6, 4, 2)] + [kv_two]

    rows = by_core(
        first, half_of(out_proj, core), moved(half_of(out_proj, 1 - core), core=True), 0
    )
    rows = in_order([rows, moved(rows, z=1), moved(rows, z=2), moved(rows, z=3)], lax.axis_index("z"))
    rows = in_order([rows, moved(rows, x=1), moved(rows, x=2), moved(rows, x=3)], lax.axis_index("x"))

    chip_block = lax.axis_index(AXES) - core
    seen = lax.dynamic_slice_in_dim(visible, chip_block, 2, 0)
    attended = attend(seen, query_two, windows).reshape(4, 2 * tokens, -1)

    sums = []
    for step in (2, 1, 3, 0):
        piece = lax.dynamic_index_in_dim(attended, (place_y + step) % 4, 0, keepdims=False)
        piece = moved(piece, y=step) if step else piece
        full = by_core(first, piece, moved(piece, core=True), 1)
        part = jnp.dot(full, rows, preferred_element_type=jnp.float32).astype(jnp.bfloat16)
        sums.append(moved(part, y=-step) if step else part)
    summed = sum(part.astype(jnp.float32) for part in sums).astype(jnp.bfloat16)
    summed = summed.reshape(2, tokens, -1)
    keep = lax.dynamic_index_in_dim(summed, core, 0, keepdims=False)
    give = lax.dynamic_index_in_dim(summed, 1 - core, 0, keepdims=False)
    projected = by_core(first, keep, moved(give, core=True), 1).astype(jnp.float32)

    hidden_sum = residual.astype(jnp.float32) + projected
    mean_square = jnp.mean(hidden_sum * hidden_sum, axis=-1, keepdims=True)
    normed = (hidden_sum * lax.rsqrt(mean_square + 1e-05) * norm_gain).astype(jnp.bfloat16)

    window_experts = expert_gate.shape[0]
    choose = expert_ids[None] == jnp.arange(window_experts, dtype=jnp.int32)[:, None, None]
    member = jnp.any(choose, axis=2)
    token_weight = jnp.sum(jnp.where(choose, route_weight[None], 0.0), axis=2)
    ranked = jnp.cumsum(member.astype(jnp.int32), axis=1) - member.astype(jnp.int32)
    slot_hit = (
        ranked[:, None, :] == jnp.arange(CAP, dtype=jnp.int32)[None, :, None]
    ) & member[:, None, :]
    dispatch = slot_hit.astype(jnp.bfloat16)
    outgoing = jnp.einsum(
        "wct,td->wcd", dispatch, normed, preferred_element_type=jnp.float32
    ).astype(jnp.bfloat16)
    combine = jnp.where(slot_hit, token_weight[:, None, :], 0.0)

    own = outgoing
    flip = moved(own, y=2)
    up1, up3, up2 = moved(own, z=1), moved(own, z=3), moved(own, z=2)
    flip1, flip3, flip2 = moved(flip, z=1), moved(flip, z=3), moved(up2, y=2)
    pieces = [own, up1, up2, up3, flip, flip1, flip2, flip3]
    pieces = pieces + [moved(piece, core=True) for piece in pieces]
    slots = jnp.concatenate(pieces, axis=1)
    gate_act = jnp.einsum("wnd,wfd->wnf", slots, expert_gate, preferred_element_type=jnp.float32)
    up_act = jnp.einsum("wnd,wfd->wnf", slots, expert_up, preferred_element_type=jnp.float32)
    activated = (jax.nn.silu(gate_act) * up_act).astype(jnp.bfloat16)
    partial_value = jnp.einsum(
        "wnf,wfd->wnd", activated, expert_down, preferred_element_type=jnp.float32
    ).astype(jnp.bfloat16)

    count = 8 * CAP
    def total(*terms):
        return sum(term.astype(jnp.float32) for term in terms).astype(jnp.bfloat16)

    crossed = moved(partial_value[:, count:], core=True)
    owed = [
        total(
            partial_value[:, place * CAP : (place + 1) * CAP],
            crossed[:, place * CAP : (place + 1) * CAP],
        )
        for place in range(8)
    ]
    far = moved(owed[6], y=2)
    side1 = moved(owed[5], z=3)
    side3 = moved(owed[7], z=1)
    near1 = moved(owed[1], z=3)
    near3 = moved(owed[3], z=1)
    across = moved(total(owed[4], side1, side3), y=2)
    twice = moved(total(owed[2], far), z=2)
    returned = sum(t.astype(jnp.float32) for t in (owed[0], near1, near3, across, twice))
    expert_mix = jnp.einsum("wct,wcd->td", combine, returned, precision=lax.Precision.HIGHEST)
    return (hidden_sum + expert_mix).astype(jnp.bfloat16)


def solution(mesh):
    finer = Mesh(mesh.devices.reshape(SIZES), AXES)
    in_specs = (
        P(AXES, None),
        P(AXES, None),
        P(AXES, None),
        P(AXES, None),
        P(),
        P(AXES, None),
        P(),
        P(AXES, None),
        P(AXES, None),
        P(None, EP, None),
        P(None, EP, None),
        P(None, EP, None),
    )
    return jax.shard_map(
        local, mesh=finer, in_specs=in_specs, out_specs=P(AXES, None), check_vma=False
    )
```

```python
import math

import jax
import jax.numpy as jnp
from jax import lax
from jax.experimental import pallas as pl
from jax.experimental.pallas import tpu as pltpu
from jax.sharding import Mesh
from jax.sharding import PartitionSpec as P

HEAD = 128
CAP = 40
SIZES = (4, 2, 4, 2, 2)
AXES = ("x", "yl", "z", "h", "c")
EP = ("z", "h", "c")


def flat(coords):
    place = 0
    for size, coord in zip(SIZES, coords):
        place = place * size + coord
    return place


def sent(value, rule):
    pairs = []
    for source in range(math.prod(SIZES)):
        rest, coords = source, []
        for size in reversed(SIZES):
            coords.append(rest % size)
            rest //= size
        cx, cyl, cz, ch, cc = reversed(coords)
        x, y, z, core = rule(cx, 2 * ch + cyl, cz, cc)
        pairs.append((source, flat((x % 4, y % 2, z % 4, y % 4 // 2, core))))
    return lax.ppermute(value, AXES, pairs)


def moved(value, x=0, y=0, z=0):
    return sent(value, lambda cx, cy, cz, cc: (cx + x, cy + y, cz + z, cc))


def crossed(value):
    return sent(value, lambda cx, cy, cz, cc: (cx, cy, cz, 1 - cc))


def mate(place, pairing):
    return place + (1 if (place + pairing) % 2 == 0 else -1)


def to_mate(value, along_x, along_z, switch):
    def rule(cx, cy, cz, cc):
        goal = 1 - cc if switch else cc
        return (mate(cx, goal) if along_x else cx, cy, mate(cz, goal) if along_z else cz, goal)

    return sent(value, rule)


def from_mate(value, along_x, along_z, switch):
    def rule(cx, cy, cz, cc):
        goal = 1 - cc if switch else cc
        return (mate(cx, cc) if along_x else cx, cy, mate(cz, cc) if along_z else cz, goal)

    return sent(value, rule)


def later(value, blocks):
    count = math.prod(SIZES)
    return lax.ppermute(value, AXES, [(s, s + blocks) for s in range(count - blocks)])


def half_of(value, which):
    width = value.shape[-1] // 2
    return lax.dynamic_slice_in_dim(value, which * width, width, value.ndim - 1)


def by_core(first, own, other, axis):
    return jnp.where(
        first,
        jnp.concatenate([own, other], axis=axis),
        jnp.concatenate([other, own], axis=axis),
    )


def attend_kernel(seen_ref, query_ref, *refs):
    key_refs, value_refs, out_ref = refs[:5], refs[5:10], refs[10]
    keys = jnp.concatenate([ref[...] for ref in key_refs], axis=0)
    values = jnp.concatenate([ref[...] for ref in value_refs], axis=0)
    factor = math.log2(math.e) / math.sqrt(HEAD)
    tokens = 128
    row = lax.broadcasted_iota(jnp.int32, (tokens, tokens), 0)
    col = lax.broadcasted_iota(jnp.int32, (tokens, tokens), 1)
    causal = jnp.where(col <= row, 0.0, -1e30)
    for block in range(2):
        here = slice(block * tokens, (block + 1) * tokens)
        key_window = keys[block * tokens : (block + 9) * tokens]
        value_window = values[block * tokens : (block + 9) * tokens]
        hidden = [
            jnp.full((tokens, tokens), jnp.where(seen_ref[block, 8 - place] > 0, 0.0, -1e30))
            for place in range(8)
        ]
        bias = jnp.concatenate(hidden + [causal], axis=1)
        query = jnp.concatenate(
            [query_ref[here, head * HEAD : (head + 1) * HEAD] for head in range(4)], axis=0
        )
        scores = lax.dot_general(
            query, key_window, (((1,), (1,)), ((), ())), preferred_element_type=jnp.float32
        )
        weights, totals = [], []
        for head in range(4):
            score = scores[head * tokens : (head + 1) * tokens] + bias
            peak = jnp.max(score, axis=1, keepdims=True)
            weight = jnp.exp2((score - peak) * factor)
            totals.append(jnp.sum(weight, axis=1, keepdims=True))
            weights.append(weight.astype(jnp.bfloat16))
        mixed = jnp.dot(
            jnp.concatenate(weights, axis=0), value_window, preferred_element_type=jnp.float32
        )
        for head in range(4):
            result = mixed[head * tokens : (head + 1) * tokens] / totals[head]
            lanes = slice(head // 2 * HEAD, head // 2 * HEAD + HEAD)
            out_ref[0, head % 2, here, lanes] = result.astype(jnp.bfloat16)


def attend(seen, query, windows):
    key_specs = [pl.BlockSpec((256, HEAD), lambda j: (0, j)) for _ in windows]
    value_specs = [pl.BlockSpec((256, HEAD), lambda j: (0, 4 + j)) for _ in windows]
    return pl.pallas_call(
        attend_kernel,
        grid=(4,),
        in_specs=[
            pl.BlockSpec(memory_space=pltpu.SMEM),
            pl.BlockSpec((256, 4 * HEAD), lambda j: (0, j)),
            *key_specs,
            *value_specs,
        ],
        out_specs=pl.BlockSpec((1, 2, 256, 256), lambda j: (j // 2, 0, 0, j % 2)),
        out_shape=jax.ShapeDtypeStruct((2, 2, 256, 512), jnp.bfloat16),
        name="attend",
        cost_estimate=pl.CostEstimate(
            flops=6_000_000_000, transcendentals=5_000_000, bytes_accessed=6_000_000
        ),
    )(seen, query, *windows, *windows)


def in_order(pieces, own_index):
    count = len(pieces)
    table = jnp.zeros((count, *pieces[0].shape), pieces[0].dtype)
    for step, piece in enumerate(pieces):
        table = lax.dynamic_update_index_in_dim(table, piece, (own_index - step) % count, 0)
    return table


def project_kernel(core_ref, *refs):
    mine, mine_other, theirs, theirs_other, rows_own, rows_other, straight_ref, switch_ref = refs
    left = jnp.concatenate([mine[0], mine_other[0]], axis=0)
    right = jnp.concatenate([theirs[0], theirs_other[0]], axis=0)
    product = jnp.dot(left, rows_own[0], preferred_element_type=jnp.float32)
    product += jnp.dot(right, rows_other[0], preferred_element_type=jnp.float32)
    product = product.astype(jnp.bfloat16)
    straight_ref[...] = product[:128]
    switch_ref[...] = product[128:]


def project(core, own_heads, other_heads, rows):
    columns = 512
    own_heads = own_heads.reshape(2, 128, 512)
    other_heads = other_heads.reshape(2, 128, 512)
    here = pl.BlockSpec((1, 128, 512), lambda n, core: (core[0], 0, 0))
    there = pl.BlockSpec((1, 128, 512), lambda n, core: (1 - core[0], 0, 0))
    out = pl.BlockSpec((128, columns), lambda n, core: (0, n))
    shape = jax.ShapeDtypeStruct((128, rows.shape[2]), jnp.bfloat16)
    return pl.pallas_call(
        project_kernel,
        grid_spec=pltpu.PrefetchScalarGridSpec(
            num_scalar_prefetch=1,
            grid=(rows.shape[2] // columns,),
            in_specs=[
                here,
                there,
                here,
                there,
                pl.BlockSpec((1, 512, columns), lambda n, core: (core[0], 0, n)),
                pl.BlockSpec((1, 512, columns), lambda n, core: (1 - core[0], 0, n)),
            ],
            out_specs=[out, out],
        ),
        out_shape=[shape, shape],
        name="project",
        cost_estimate=pl.CostEstimate(
            flops=1_073_741_824, transcendentals=0, bytes_accessed=6_000_000
        ),
    )(core.reshape(1), own_heads, own_heads, other_heads, other_heads, rows, rows)


def expert_kernel(*refs):
    slot_refs, (gate_ref, up_ref, down_ref, own_ref, other_ref) = refs[:16], refs[16:21]
    gate_sum, up_sum, act = refs[21:]
    step = pl.program_id(0)
    contract = (((1,), (1,)), ((), ()))

    @pl.when(step < 4)
    def _():
        slots = jnp.concatenate([ref[...] for ref in slot_refs], axis=0)
        gate = lax.dot_general(slots, gate_ref[0], contract, preferred_element_type=jnp.float32)
        up = lax.dot_general(slots, up_ref[0], contract, preferred_element_type=jnp.float32)

        @pl.when(step == 0)
        def _():
            gate_sum[...] = gate
            up_sum[...] = up

        @pl.when(step > 0)
        def _():
            gate_sum[...] += gate
            up_sum[...] += up

        @pl.when(step == 3)
        def _():
            value = gate_sum[...]
            act[...] = (value / (1.0 + jnp.exp(-value)) * up_sum[...]).astype(jnp.bfloat16)

    @pl.when(step >= 4)
    def _():
        result = jnp.dot(act[...], down_ref[0], preferred_element_type=jnp.float32)
        result = result.astype(jnp.bfloat16)
        half = result.shape[0] // 2
        own_ref[...] = result[:half]
        other_ref[...] = result[half:]


def expert(which, pieces, gate, up, down):
    slots, width = pieces[0].shape
    hidden = gate.shape[1]
    chunk = width // 4
    count = len(pieces) * slots
    early = lambda step: jnp.minimum(step, 3)
    late = lambda step: jnp.maximum(step - 4, 0)
    out = pl.BlockSpec((count // 2, chunk), lambda step: (0, late(step)))
    shape = jax.ShapeDtypeStruct((count // 2, width), jnp.bfloat16)
    return pl.pallas_call(
        expert_kernel,
        grid=(8,),
        in_specs=[
            *[pl.BlockSpec((slots, chunk), lambda step: (0, early(step))) for _ in pieces],
            pl.BlockSpec((1, hidden, chunk), lambda step: (which, 0, early(step))),
            pl.BlockSpec((1, hidden, chunk), lambda step: (which, 0, early(step))),
            pl.BlockSpec((1, hidden, chunk), lambda step: (which, 0, late(step))),
        ],
        out_specs=[out, out],
        out_shape=[shape, shape],
        scratch_shapes=[
            pltpu.VMEM((count, hidden), jnp.float32),
            pltpu.VMEM((count, hidden), jnp.float32),
            pltpu.VMEM((count, hidden), jnp.bfloat16),
        ],
        name="expert",
        cost_estimate=pl.CostEstimate(
            flops=7_000_000_000, transcendentals=300_000, bytes_accessed=22_000_000
        ),
    )(*pieces, gate, up, down)


def total(*terms):
    return sum(term.astype(jnp.float32) for term in terms).astype(jnp.bfloat16)


def gather_slots(own):
    flip = moved(own, y=2)
    up1, up3, up2 = moved(own, z=1), moved(own, z=3), moved(own, z=2)
    flip1, flip3, flip2 = moved(flip, z=1), moved(flip, z=3), moved(up2, y=2)
    pieces = [own, up1, up2, up3, flip, flip1, flip2, flip3]
    return pieces + [crossed(piece) for piece in pieces]


def return_sums(own_part, other_part):
    swapped = crossed(other_part)

    def owed(place):
        rows = slice(place * CAP, (place + 1) * CAP)
        return total(own_part[rows], swapped[rows])

    side1, side3 = moved(owed(5), z=3), moved(owed(7), z=1)
    far = moved(owed(6), y=2)
    near1, near3 = moved(owed(1), z=3), moved(owed(3), z=1)
    across = moved(total(owed(4), side1, side3), y=2)
    twice = moved(total(owed(2), far), z=2)
    return sum(t.astype(jnp.float32) for t in (owed(0), near1, near3, across, twice))


def local(
    residual,
    queries,
    key_rows,
    value_rows,
    visible,
    out_proj,
    norm_gain,
    expert_ids,
    route_weight,
    expert_gate,
    expert_up,
    expert_down,
):
    core = lax.axis_index("c")
    first = core == 0
    tokens = residual.shape[0]
    place_x, place_z = lax.axis_index("x"), lax.axis_index("z")
    place_y = 2 * lax.axis_index("h") + lax.axis_index("yl")

    kv_own = jnp.concatenate([half_of(key_rows, core), half_of(value_rows, core)], axis=1)
    kv_give = jnp.concatenate([half_of(key_rows, 1 - core), half_of(value_rows, 1 - core)], axis=1)
    kv_two = by_core(first, kv_own, crossed(kv_give), 0)
    query_two = by_core(first, half_of(queries, core), crossed(half_of(queries, 1 - core)), 0)
    windows = [later(kv_two, blocks) for blocks in (8, 6, 4, 2)] + [kv_two]

    columns = out_proj.shape[1] // 2
    rows = by_core(first, half_of(out_proj, core), crossed(half_of(out_proj, 1 - core)), 0)
    rows = in_order([rows, moved(rows, z=2)], place_z // 2)
    rows = in_order([rows] + [moved(rows, y=step) for step in (1, 2, 3)], place_y)
    rows = rows.reshape(2, 2, 2, 2 * out_proj.shape[0], columns)
    rows = rows.transpose(1, 2, 0, 3, 4).reshape(-1, columns)
    rows = in_order([rows, moved(rows, x=2)], place_x // 2)

    chip_block = lax.axis_index(AXES) - core
    seen = lax.dynamic_slice_in_dim(visible, chip_block, 2, 0)
    attended = attend(seen, query_two, windows)
    attended = attended.reshape(4, 2 * tokens, -1)

    straight, switched = [], []
    for along_x, along_z in ((1, 1), (1, 0), (0, 1), (0, 0)):
        wanted = (place_x % 2 ^ along_x) * 2 + (place_z % 2 ^ along_z)
        piece = lax.dynamic_index_in_dim(attended, wanted, 0, keepdims=False)
        if along_x or along_z:
            same = to_mate(piece, along_x, along_z, False)
            other = to_mate(piece, along_x, along_z, True)
        else:
            same, other = piece, crossed(piece)
        here, there = project(core, same, other, rows)
        if along_x or along_z:
            here = from_mate(here, along_x, along_z, False)
            there = from_mate(there, along_x, along_z, True)
        else:
            there = crossed(there)
        straight.append(here.astype(jnp.float32))
        switched.append(there.astype(jnp.float32))
    projected = by_core(first, sum(straight), sum(switched), 1)

    hidden_sum = residual.astype(jnp.float32) + projected
    mean_square = jnp.mean(hidden_sum * hidden_sum, axis=-1, keepdims=True)
    normed = (hidden_sum * lax.rsqrt(mean_square + 1e-05) * norm_gain).astype(jnp.bfloat16)

    mixes, slots = [], []
    for which in range(expert_gate.shape[0]):
        choose = expert_ids == which
        member = jnp.any(choose, axis=1)
        token_weight = jnp.sum(jnp.where(choose, route_weight, 0.0), axis=1)
        ranked = jnp.cumsum(member.astype(jnp.int32)) - member.astype(jnp.int32)
        slot_hit = (ranked[None, :] == jnp.arange(CAP, dtype=jnp.int32)[:, None]) & member[None, :]
        slots.append(slot_hit.astype(jnp.bfloat16))
        mixes.append(jnp.where(slot_hit, token_weight[None, :], 0.0))
    outgoing = jnp.dot(
        jnp.concatenate(slots, axis=0), normed, preferred_element_type=jnp.float32
    ).astype(jnp.bfloat16)

    returned, held = [], outgoing
    for which in range(expert_gate.shape[0]):
        own = held[which * CAP : (which + 1) * CAP]
        pieces = gather_slots(own)
        if which == 0:
            held, pieces[4] = lax.optimization_barrier((held, pieces[4]))
        own_part, other_part = expert(which, pieces, expert_gate, expert_up, expert_down)
        returned.append(return_sums(own_part, other_part))
    expert_mix = jnp.dot(
        jnp.concatenate(mixes, axis=0).T,
        jnp.concatenate(returned, axis=0),
        precision=lax.Precision.HIGHEST,
    )
    return (hidden_sum + expert_mix).astype(jnp.bfloat16)


def solution(mesh):
    finer = Mesh(mesh.devices.reshape(SIZES), AXES)
    in_specs = (
        P(AXES, None),
        P(AXES, None),
        P(AXES, None),
        P(AXES, None),
        P(),
        P(AXES, None),
        P(),
        P(AXES, None),
        P(AXES, None),
        P(None, EP, None),
        P(None, EP, None),
        P(None, EP, None),
    )
    return jax.shard_map(
        local, mesh=finer, in_specs=in_specs, out_specs=P(AXES, None), check_vma=False
    )
```

```python
import math

import jax
import jax.numpy as jnp
from jax import lax
from jax.experimental import pallas as pl
from jax.experimental.pallas import tpu as pltpu
from jax.sharding import Mesh
from jax.sharding import PartitionSpec as P


HEAD = 128
CAP = 40
SIZES = (4, 2, 4, 2, 2)
AXES = ("x", "yl", "z", "h", "c")
EP = ("z", "h", "c")


def flat(coords):
    place = 0
    for size, coord in zip(SIZES, coords):
        place = place * size + coord
    return place


def sent(value, rule):
    pairs = []
    for source in range(math.prod(SIZES)):
        rest, coords = source, []
        for size in reversed(SIZES):
            coords.append(rest % size)
            rest //= size
        cx, cyl, cz, ch, cc = reversed(coords)
        x, y, z, core = rule(cx, 2 * ch + cyl, cz, cc)
        pairs.append((source, flat((x % 4, y % 2, z % 4, y % 4 // 2, core))))
    return lax.ppermute(value, AXES, pairs)


def moved(value, x=0, y=0, z=0):
    return sent(value, lambda cx, cy, cz, cc: (cx + x, cy + y, cz + z, cc))


def crossed(value):
    return sent(value, lambda cx, cy, cz, cc: (cx, cy, cz, 1 - cc))


def mate(place, pairing):
    return place + (1 if (place + pairing) % 2 == 0 else -1)


def to_mate(value, along_x, along_z, switch):
    def rule(cx, cy, cz, cc):
        goal = 1 - cc if switch else cc
        return (mate(cx, goal) if along_x else cx, cy, mate(cz, goal) if along_z else cz, goal)

    return sent(value, rule)


def from_mate(value, along_x, along_z, switch):
    def rule(cx, cy, cz, cc):
        goal = 1 - cc if switch else cc
        return (mate(cx, cc) if along_x else cx, cy, mate(cz, cc) if along_z else cz, goal)

    return sent(value, rule)


def later(value, blocks):
    count = math.prod(SIZES)
    return lax.ppermute(value, AXES, [(s, s + blocks) for s in range(count - blocks)])


def half_of(value, which):
    width = value.shape[-1] // 2
    return lax.dynamic_slice_in_dim(value, which * width, width, value.ndim - 1)


def by_core(first, own, other, axis):
    return jnp.where(
        first,
        jnp.concatenate([own, other], axis=axis),
        jnp.concatenate([other, own], axis=axis),
    )


def attend_kernel(seen_ref, query_ref, *refs):
    key_refs, value_refs, out_ref = refs[:5], refs[5:10], refs[10]
    keys = jnp.concatenate([ref[...] for ref in key_refs], axis=0)
    values = jnp.concatenate([ref[...] for ref in value_refs], axis=0)
    factor = math.log2(math.e) / math.sqrt(HEAD)
    tokens = 128
    row = lax.broadcasted_iota(jnp.int32, (tokens, tokens), 0)
    col = lax.broadcasted_iota(jnp.int32, (tokens, tokens), 1)
    causal = jnp.where(col <= row, 0.0, -1e30)
    for block in range(2):
        here = slice(block * tokens, (block + 1) * tokens)
        key_window = keys[block * tokens : (block + 9) * tokens]
        value_window = values[block * tokens : (block + 9) * tokens]
        hidden = [
            jnp.full((tokens, tokens), jnp.where(seen_ref[block, 8 - place] > 0, 0.0, -1e30))
            for place in range(8)
        ]
        bias = jnp.concatenate(hidden + [causal], axis=1)
        query = jnp.concatenate(
            [query_ref[here, head * HEAD : (head + 1) * HEAD] for head in range(4)], axis=0
        )
        scores = lax.dot_general(
            query, key_window, (((1,), (1,)), ((), ())), preferred_element_type=jnp.float32
        )
        weights, totals = [], []
        for head in range(4):
            score = scores[head * tokens : (head + 1) * tokens] + bias
            peak = jnp.max(score, axis=1, keepdims=True)
            weight = jnp.exp2((score - peak) * factor)
            totals.append(jnp.sum(weight, axis=1, keepdims=True))
            weights.append(weight.astype(jnp.bfloat16))
        mixed = jnp.dot(
            jnp.concatenate(weights, axis=0), value_window, preferred_element_type=jnp.float32
        )
        for head in range(4):
            result = mixed[head * tokens : (head + 1) * tokens] / totals[head]
            lanes = slice(head // 2 * HEAD, head // 2 * HEAD + HEAD)
            out_ref[0, head % 2, here, lanes] = result.astype(jnp.bfloat16)


def attend(seen, query, windows):
    key_specs = [pl.BlockSpec((256, HEAD), lambda j: (0, j)) for _ in windows]
    value_specs = [pl.BlockSpec((256, HEAD), lambda j: (0, 4 + j)) for _ in windows]
    return pl.pallas_call(
        attend_kernel,
        grid=(4,),
        in_specs=[
            pl.BlockSpec(memory_space=pltpu.SMEM),
            pl.BlockSpec((256, 4 * HEAD), lambda j: (0, j)),
            *key_specs,
            *value_specs,
        ],
        out_specs=pl.BlockSpec((1, 2, 256, 256), lambda j: (j // 2, 0, 0, j % 2)),
        out_shape=jax.ShapeDtypeStruct((2, 2, 256, 512), jnp.bfloat16),
        name="attend",
        cost_estimate=pl.CostEstimate(
            flops=6_000_000_000, transcendentals=5_000_000, bytes_accessed=6_000_000
        ),
    )(seen, query, *windows, *windows)


def in_order(pieces, own_index):
    count = len(pieces)
    table = jnp.zeros((count, *pieces[0].shape), pieces[0].dtype)
    for step, piece in enumerate(pieces):
        table = lax.dynamic_update_index_in_dim(table, piece, (own_index - step) % count, 0)
    return table


def project_kernel(core_ref, *refs):
    same, other, (rows_own, rows_other) = refs[:8], refs[8:16], refs[16:18]
    left = jnp.concatenate([ref[0] for ref in same], axis=0)
    right = jnp.concatenate([ref[0] for ref in other], axis=0)
    product = jnp.dot(left, rows_own[0], preferred_element_type=jnp.float32)
    product += jnp.dot(right, rows_other[0], preferred_element_type=jnp.float32)
    product = product.astype(jnp.bfloat16)
    for place, out_ref in enumerate(refs[18:]):
        out_ref[...] = product[place * 128 : (place + 1) * 128]


def project(core, same, other, rows):
    columns = 512
    same = [heads.reshape(2, 128, 512) for heads in same for _ in range(2)]
    other = [heads.reshape(2, 128, 512) for heads in other for _ in range(2)]
    here = pl.BlockSpec((1, 128, 512), lambda n, core: (core[0], 0, 0))
    there = pl.BlockSpec((1, 128, 512), lambda n, core: (1 - core[0], 0, 0))
    out = pl.BlockSpec((128, columns), lambda n, core: (0, n))
    shape = jax.ShapeDtypeStruct((128, rows.shape[2]), jnp.bfloat16)
    return pl.pallas_call(
        project_kernel,
        grid_spec=pltpu.PrefetchScalarGridSpec(
            num_scalar_prefetch=1,
            grid=(rows.shape[2] // columns,),
            in_specs=[
                *[here, there] * 8,
                pl.BlockSpec((1, 512, columns), lambda n, core: (core[0], 0, n)),
                pl.BlockSpec((1, 512, columns), lambda n, core: (1 - core[0], 0, n)),
            ],
            out_specs=[out] * 8,
        ),
        out_shape=[shape] * 8,
        name="project",
        cost_estimate=pl.CostEstimate(
            flops=4_300_000_000, transcendentals=0, bytes_accessed=10_000_000
        ),
    )(core.reshape(1), *same, *other, rows, rows)


def expert_kernel(*refs):
    slot_refs, (gate_ref, up_ref, down_ref, own_ref, other_ref) = refs[:4], refs[4:9]
    gate_sum, up_sum, act = refs[9:]
    step = pl.program_id(1)
    contract = (((1,), (1,)), ((), ()))

    @pl.when(step < 4)
    def _():
        slots = jnp.concatenate([ref[0] for ref in slot_refs], axis=0)
        gate = lax.dot_general(slots, gate_ref[0], contract, preferred_element_type=jnp.float32)
        up = lax.dot_general(slots, up_ref[0], contract, preferred_element_type=jnp.float32)

        @pl.when(step == 0)
        def _():
            gate_sum[...] = gate
            up_sum[...] = up

        @pl.when(step > 0)
        def _():
            gate_sum[...] += gate
            up_sum[...] += up

        @pl.when(step == 3)
        def _():
            value = gate_sum[...]
            act[...] = (value / (1.0 + jnp.exp(-value)) * up_sum[...]).astype(jnp.bfloat16)

    @pl.when(step >= 4)
    def _():
        result = jnp.dot(act[...], down_ref[0], preferred_element_type=jnp.float32)
        result = result.astype(jnp.bfloat16)
        half = result.shape[0] // 2
        own_ref[0] = result[:half]
        other_ref[0] = result[half:]


def experts(pieces, gate, up, down):
    count, slots, width = pieces[0].shape
    hidden = gate.shape[1]
    chunk = width // 4
    rows = len(pieces) * slots
    early = lambda e, step: (e, 0, jnp.minimum(step, 3))
    late = lambda e, step: (e, 0, jnp.maximum(step - 4, 0))
    out = pl.BlockSpec((1, rows // 2, chunk), late)
    shape = jax.ShapeDtypeStruct((count, rows // 2, width), jnp.bfloat16)
    return pl.pallas_call(
        expert_kernel,
        grid=(count, 8),
        in_specs=[
            *[pl.BlockSpec((1, slots, chunk), early) for _ in pieces],
            pl.BlockSpec((1, hidden, chunk), early),
            pl.BlockSpec((1, hidden, chunk), early),
            pl.BlockSpec((1, hidden, chunk), late),
        ],
        out_specs=[out, out],
        out_shape=[shape, shape],
        scratch_shapes=[
            pltpu.VMEM((rows, hidden), jnp.float32),
            pltpu.VMEM((rows, hidden), jnp.float32),
            pltpu.VMEM((rows, hidden), jnp.bfloat16),
        ],
        name="experts",
        cost_estimate=pl.CostEstimate(
            flops=14_000_000_000, transcendentals=600_000, bytes_accessed=44_000_000
        ),
    )(*pieces, gate, up, down)


def total(*terms):
    return sum(term.astype(jnp.float32) for term in terms).astype(jnp.bfloat16)


def gather_slots(own):
    flip = moved(own, y=2)
    up2, up1, up3 = moved(own, z=2), moved(own, z=1), moved(own, z=3)
    flip1, flip3, flip2 = moved(flip, z=1), moved(flip, z=3), moved(up2, y=2)
    early = jnp.concatenate([own, up1, up3, flip], axis=1)
    late = jnp.concatenate([up2, flip1, flip3, flip2], axis=1)
    return [early, late, crossed(early), crossed(late)]


def return_sums(own_part, other_part):
    swapped = crossed(other_part)

    def owed(place):
        rows = slice(place * CAP, (place + 1) * CAP)
        return total(own_part[:, rows], swapped[:, rows])

    own, up1, up3, flip, up2, flip1, flip3, flip2 = [owed(place) for place in range(8)]
    side1, side3 = moved(flip1, z=3), moved(flip3, z=1)
    far = moved(flip2, y=2)
    near1, near3 = moved(up1, z=3), moved(up3, z=1)
    across = moved(total(flip, side1, side3), y=2)
    twice = moved(total(up2, far), z=2)
    return sum(t.astype(jnp.float32) for t in (own, near1, near3, across, twice))


def local(
    residual,
    queries,
    key_rows,
    value_rows,
    visible,
    out_proj,
    norm_gain,
    expert_ids,
    route_weight,
    expert_gate,
    expert_up,
    expert_down,
):
    core = lax.axis_index("c")
    first = core == 0
    tokens = residual.shape[0]
    place_x, place_z = lax.axis_index("x"), lax.axis_index("z")
    place_y = 2 * lax.axis_index("h") + lax.axis_index("yl")

    kv_own = jnp.concatenate([half_of(key_rows, core), half_of(value_rows, core)], axis=1)
    kv_give = jnp.concatenate([half_of(key_rows, 1 - core), half_of(value_rows, 1 - core)], axis=1)
    kv_got = crossed(kv_give)
    kv_two = by_core(first, kv_own, kv_got, 0)
    query_got = crossed(half_of(queries, 1 - core))
    query_two = by_core(first, half_of(queries, core), query_got, 0)
    windows = [later(kv_two, blocks) for blocks in (8, 6, 4, 2)] + [kv_two]

    columns = out_proj.shape[1] // 2
    rows_got = crossed(half_of(out_proj, 1 - core))
    rows = by_core(first, half_of(out_proj, core), rows_got, 0)
    rows_got = moved(rows, z=2)
    rows = in_order([rows, rows_got], place_z // 2)
    rows_got = [moved(rows, y=step) for step in (1, 2, 3)]
    rows = in_order([rows, *rows_got], place_y)
    rows = rows.reshape(2, 2, 2, 2 * out_proj.shape[0], columns)
    rows = rows.transpose(1, 2, 0, 3, 4).reshape(-1, columns)
    rows_got = moved(rows, x=2)
    rows = in_order([rows, rows_got], place_x // 2)

    chip_block = lax.axis_index(AXES) - core
    seen = lax.dynamic_slice_in_dim(visible, chip_block, 2, 0)
    attended = attend(seen, query_two, windows)
    attended = attended.reshape(4, 2 * tokens, -1)

    ways = ((1, 1), (1, 0), (0, 1), (0, 0))
    same, other = [], []
    for along_x, along_z in ways:
        wanted = (place_x % 2 ^ along_x) * 2 + (place_z % 2 ^ along_z)
        piece = lax.dynamic_index_in_dim(attended, wanted, 0, keepdims=False)
        remote = along_x or along_z
        same.append(to_mate(piece, along_x, along_z, False) if remote else piece)
        other.append(to_mate(piece, along_x, along_z, True) if remote else crossed(piece))
    products = project(core, same, other, rows)
    straight, switched = [], []
    for place, (along_x, along_z) in enumerate(ways):
        here, there = products[2 * place : 2 * place + 2]
        if along_x or along_z:
            here = from_mate(here, along_x, along_z, False)
            there = from_mate(there, along_x, along_z, True)
        else:
            there = crossed(there)
        straight.append(here.astype(jnp.float32))
        switched.append(there.astype(jnp.float32))
    projected = by_core(first, sum(straight), sum(switched), 1)

    hidden_sum = residual.astype(jnp.float32) + projected
    mean_square = jnp.mean(hidden_sum * hidden_sum, axis=-1, keepdims=True)
    normed = (hidden_sum * lax.rsqrt(mean_square + 1e-05) * norm_gain).astype(jnp.bfloat16)

    mixes, slots = [], []
    for which in range(expert_gate.shape[0]):
        choose = expert_ids == which
        member = jnp.any(choose, axis=1)
        token_weight = jnp.sum(jnp.where(choose, route_weight, 0.0), axis=1)
        ranked = jnp.cumsum(member.astype(jnp.int32)) - member.astype(jnp.int32)
        slot_hit = (ranked[None, :] == jnp.arange(CAP, dtype=jnp.int32)[:, None]) & member[None, :]
        slots.append(slot_hit.astype(jnp.bfloat16))
        mixes.append(jnp.where(slot_hit, token_weight[None, :], 0.0))
    outgoing = jnp.dot(
        jnp.concatenate(slots, axis=0), normed, preferred_element_type=jnp.float32
    ).astype(jnp.bfloat16)

    pieces = gather_slots(outgoing.reshape(-1, CAP, outgoing.shape[1]))
    returned = return_sums(*experts(pieces, expert_gate, expert_up, expert_down))
    expert_mix = jnp.dot(
        jnp.concatenate(mixes, axis=0).T,
        returned.reshape(-1, returned.shape[2]),
        precision=lax.Precision.HIGHEST,
    )
    return (hidden_sum + expert_mix).astype(jnp.bfloat16)


def solution(mesh):
    finer = Mesh(mesh.devices.reshape(SIZES), AXES)
    in_specs = (
        P(AXES, None),
        P(AXES, None),
        P(AXES, None),
        P(AXES, None),
        P(),
        P(AXES, None),
        P(),
        P(AXES, None),
        P(AXES, None),
        P(None, EP, None),
        P(None, EP, None),
        P(None, EP, None),
    )
    return jax.shard_map(
        local, mesh=finer, in_specs=in_specs, out_specs=P(AXES, None), check_vma=False
    )
```

```python
import math

import jax
import jax.numpy as jnp
from jax import lax
from jax.experimental import pallas as pl
from jax.experimental.pallas import tpu as pltpu
from jax.sharding import Mesh
from jax.sharding import PartitionSpec as P


HEAD = 128
CAP = 40
SIZES = (4, 2, 4, 2, 2)
AXES = ("x", "yl", "z", "h", "c")
EP = ("z", "h", "c")


def flat(coords):
    place = 0
    for size, coord in zip(SIZES, coords):
        place = place * size + coord
    return place


def sent(value, rule):
    pairs = []
    for source in range(math.prod(SIZES)):
        rest, coords = source, []
        for size in reversed(SIZES):
            coords.append(rest % size)
            rest //= size
        cx, cyl, cz, ch, cc = reversed(coords)
        x, y, z, core = rule(cx, 2 * ch + cyl, cz, cc)
        pairs.append((source, flat((x % 4, y % 2, z % 4, y % 4 // 2, core))))
    return lax.ppermute(value, AXES, pairs)


def moved(value, x=0, y=0, z=0):
    return sent(value, lambda cx, cy, cz, cc: (cx + x, cy + y, cz + z, cc))


def crossed(value):
    return sent(value, lambda cx, cy, cz, cc: (cx, cy, cz, 1 - cc))


def mate(place, pairing):
    return place + (1 if (place + pairing) % 2 == 0 else -1)


def to_mate(value, along_x, along_z, switch):
    def rule(cx, cy, cz, cc):
        goal = 1 - cc if switch else cc
        return (mate(cx, goal) if along_x else cx, cy, mate(cz, goal) if along_z else cz, goal)

    return sent(value, rule)


def from_mate(value, along_x, along_z, switch):
    def rule(cx, cy, cz, cc):
        goal = 1 - cc if switch else cc
        return (mate(cx, cc) if along_x else cx, cy, mate(cz, cc) if along_z else cz, goal)

    return sent(value, rule)


def later(value, blocks):
    count = math.prod(SIZES)
    return lax.ppermute(value, AXES, [(s, s + blocks) for s in range(count - blocks)])


def half_of(value, which):
    width = value.shape[-1] // 2
    return lax.dynamic_slice_in_dim(value, which * width, width, value.ndim - 1)


def by_core(first, own, other, axis):
    return jnp.where(
        first,
        jnp.concatenate([own, other], axis=axis),
        jnp.concatenate([other, own], axis=axis),
    )


def attend_kernel(seen_ref, query_ref, *refs):
    key_refs, value_refs, out_ref = refs[:5], refs[5:10], refs[10]
    keys = jnp.concatenate([ref[...] for ref in key_refs], axis=0)
    values = jnp.concatenate([ref[...] for ref in value_refs], axis=0)
    factor = math.log2(math.e) / math.sqrt(HEAD)
    tokens = 128
    row = lax.broadcasted_iota(jnp.int32, (tokens, tokens), 0)
    col = lax.broadcasted_iota(jnp.int32, (tokens, tokens), 1)
    causal = jnp.where(col <= row, 0.0, -1e30)
    for block in range(2):
        here = slice(block * tokens, (block + 1) * tokens)
        key_window = keys[block * tokens : (block + 9) * tokens]
        value_window = values[block * tokens : (block + 9) * tokens]
        hidden = [
            jnp.full((tokens, tokens), jnp.where(seen_ref[block, 8 - place] > 0, 0.0, -1e30))
            for place in range(8)
        ]
        bias = jnp.concatenate(hidden + [causal], axis=1)
        query = jnp.concatenate(
            [query_ref[here, head * HEAD : (head + 1) * HEAD] for head in range(4)], axis=0
        )
        scores = lax.dot_general(
            query, key_window, (((1,), (1,)), ((), ())), preferred_element_type=jnp.float32
        )
        weights, totals = [], []
        for head in range(4):
            score = scores[head * tokens : (head + 1) * tokens] + bias
            peak = jnp.max(score, axis=1, keepdims=True)
            weight = jnp.exp2((score - peak) * factor)
            totals.append(jnp.sum(weight, axis=1, keepdims=True))
            weights.append(weight.astype(jnp.bfloat16))
        mixed = jnp.dot(
            jnp.concatenate(weights, axis=0), value_window, preferred_element_type=jnp.float32
        )
        for head in range(4):
            result = mixed[head * tokens : (head + 1) * tokens] / totals[head]
            lanes = slice(head // 2 * HEAD, head // 2 * HEAD + HEAD)
            out_ref[0, head % 2, here, lanes] = result.astype(jnp.bfloat16)


def attend(seen, query, windows):
    key_specs = [pl.BlockSpec((256, HEAD), lambda j: (0, j)) for _ in windows]
    value_specs = [pl.BlockSpec((256, HEAD), lambda j: (0, 4 + j)) for _ in windows]
    return pl.pallas_call(
        attend_kernel,
        grid=(4,),
        in_specs=[
            pl.BlockSpec(memory_space=pltpu.SMEM),
            pl.BlockSpec((256, 4 * HEAD), lambda j: (0, j)),
            *key_specs,
            *value_specs,
        ],
        out_specs=pl.BlockSpec((1, 2, 256, 256), lambda j: (j // 2, 0, 0, j % 2)),
        out_shape=jax.ShapeDtypeStruct((2, 2, 256, 512), jnp.bfloat16),
        name="attend",
        cost_estimate=pl.CostEstimate(
            flops=6_000_000_000, transcendentals=5_000_000, bytes_accessed=6_000_000
        ),
    )(seen, query, *windows, *windows)


def in_order(pieces, own_index):
    count = len(pieces)
    table = jnp.zeros((count, *pieces[0].shape), pieces[0].dtype)
    for step, piece in enumerate(pieces):
        table = lax.dynamic_update_index_in_dim(table, piece, (own_index - step) % count, 0)
    return table


def by_height(pieces, place_y):
    shape = pieces[0].shape
    lead = len(shape) - 3
    table = jnp.zeros((*shape[:lead], 2, shape[lead], 2, *shape[lead + 1 :]), pieces[0].dtype)
    for step, piece in enumerate(pieces):
        source = (place_y - step) % 4
        piece = piece.reshape(*shape[:lead], 1, shape[lead], 1, *shape[lead + 1 :])
        start = [0] * table.ndim
        start[lead], start[lead + 2] = source % 2, source // 2
        table = lax.dynamic_update_slice(table, piece, start)
    return table


def project_kernel(core_ref, *refs):
    same, other, row_refs = refs[:8], refs[8:16], refs[16:20]

    def multiply(rows_own, rows_other):
        left = jnp.concatenate([ref[0] for ref in same], axis=0)
        right = jnp.concatenate([ref[0] for ref in other], axis=0)
        product = jnp.dot(left, rows_own[0], preferred_element_type=jnp.float32)
        product += jnp.dot(right, rows_other[0], preferred_element_type=jnp.float32)
        product = product.astype(jnp.bfloat16)
        for place, out_ref in enumerate(refs[20:]):
            out_ref[...] = product[place * 128 : (place + 1) * 128]

    pl.when(pl.program_id(0) < 2)(lambda: multiply(*row_refs[:2]))
    pl.when(pl.program_id(0) >= 2)(lambda: multiply(*row_refs[2:]))


def project(core, same, other, low, high):
    columns = 512
    same = [heads.reshape(2, 128, 512) for heads in same for _ in range(2)]
    other = [heads.reshape(2, 128, 512) for heads in other for _ in range(2)]
    here = pl.BlockSpec((1, 128, 512), lambda n, core: (core[0], 0, 0))
    there = pl.BlockSpec((1, 128, 512), lambda n, core: (1 - core[0], 0, 0))
    out = pl.BlockSpec((128, columns), lambda n, core: (0, n))
    shape = jax.ShapeDtypeStruct((128, 2 * low.shape[2]), jnp.bfloat16)
    early = lambda n: jnp.minimum(n, 1)
    late = lambda n: jnp.maximum(n - 2, 0)
    return pl.pallas_call(
        project_kernel,
        grid_spec=pltpu.PrefetchScalarGridSpec(
            num_scalar_prefetch=1,
            grid=(4,),
            in_specs=[
                *[here, there] * 8,
                pl.BlockSpec((1, 512, columns), lambda n, core: (core[0], 0, early(n))),
                pl.BlockSpec((1, 512, columns), lambda n, core: (1 - core[0], 0, early(n))),
                pl.BlockSpec((1, 512, columns), lambda n, core: (core[0], 0, late(n))),
                pl.BlockSpec((1, 512, columns), lambda n, core: (1 - core[0], 0, late(n))),
            ],
            out_specs=[out] * 8,
        ),
        out_shape=[shape] * 8,
        name="project",
        cost_estimate=pl.CostEstimate(
            flops=4_300_000_000, transcendentals=0, bytes_accessed=10_000_000
        ),
    )(core.reshape(1), *same, *other, low, low, high, high)


def expert_kernel(*refs):
    slot_refs, (gate_ref, up_ref, down_ref, own_ref, other_ref) = refs[:4], refs[4:9]
    gate_sum, up_sum, act = refs[9:]
    step = pl.program_id(0)
    contract = (((1,), (1,)), ((), ()))

    @pl.when(step < 4)
    def _():
        slots = jnp.concatenate([ref[...] for ref in slot_refs], axis=0)
        gate = lax.dot_general(slots, gate_ref[0], contract, preferred_element_type=jnp.float32)
        up = lax.dot_general(slots, up_ref[0], contract, preferred_element_type=jnp.float32)

        @pl.when(step == 0)
        def _():
            gate_sum[...] = gate
            up_sum[...] = up

        @pl.when(step > 0)
        def _():
            gate_sum[...] += gate
            up_sum[...] += up

        @pl.when(step == 3)
        def _():
            value = gate_sum[...]
            act[...] = (value / (1.0 + jnp.exp(-value)) * up_sum[...]).astype(jnp.bfloat16)

    @pl.when(step >= 4)
    def _():
        result = jnp.dot(act[...], down_ref[0], preferred_element_type=jnp.float32)
        result = result.astype(jnp.bfloat16)
        half = result.shape[0] // 2
        own_ref[...] = result[:half]
        other_ref[...] = result[half:]


def expert(which, pieces, gate, up, down):
    slots, width = pieces[0].shape
    hidden = gate.shape[1]
    chunk = width // 4
    rows = len(pieces) * slots
    early = lambda step: jnp.minimum(step, 3)
    late = lambda step: jnp.maximum(step - 4, 0)
    out = pl.BlockSpec((rows // 2, chunk), lambda step: (0, late(step)))
    shape = jax.ShapeDtypeStruct((rows // 2, width), jnp.bfloat16)
    return pl.pallas_call(
        expert_kernel,
        grid=(8,),
        in_specs=[
            *[pl.BlockSpec((slots, chunk), lambda step: (0, early(step))) for _ in pieces],
            pl.BlockSpec((1, hidden, chunk), lambda step: (which, 0, early(step))),
            pl.BlockSpec((1, hidden, chunk), lambda step: (which, 0, early(step))),
            pl.BlockSpec((1, hidden, chunk), lambda step: (which, 0, late(step))),
        ],
        out_specs=[out, out],
        out_shape=[shape, shape],
        scratch_shapes=[
            pltpu.VMEM((rows, hidden), jnp.float32),
            pltpu.VMEM((rows, hidden), jnp.float32),
            pltpu.VMEM((rows, hidden), jnp.bfloat16),
        ],
        name="expert",
        cost_estimate=pl.CostEstimate(
            flops=7_000_000_000, transcendentals=300_000, bytes_accessed=22_000_000
        ),
    )(*pieces, gate, up, down)


def total(*terms):
    return sum(term.astype(jnp.float32) for term in terms).astype(jnp.bfloat16)


def gather_slots(own):
    flip = moved(own, y=2)
    up2, up1, up3 = moved(own, z=2), moved(own, z=1), moved(own, z=3)
    flip1, flip3 = moved(flip, z=1), moved(flip, z=3)
    flip2 = moved(up2, y=2)
    early = jnp.concatenate([own, up1, up3, flip], axis=0)
    late = jnp.concatenate([up2, flip1, flip3, flip2], axis=0)
    early_got = crossed(early)
    late_got = crossed(late)
    return [early, late, early_got, late_got]


def return_sums(own_part, other_part):
    swapped = crossed(other_part)

    def owed(place):
        rows = slice(place * CAP, (place + 1) * CAP)
        return total(own_part[rows], swapped[rows])

    own, up1, up3, flip, up2, flip1, flip3, flip2 = [owed(place) for place in range(8)]
    side1, side3 = moved(flip1, z=3), moved(flip3, z=1)
    far = moved(flip2, y=2)
    near1, near3 = moved(up1, z=3), moved(up3, z=1)
    across = moved(total(flip, side1, side3), y=2)
    twice = moved(total(up2, far), z=2)
    return sum(t.astype(jnp.float32) for t in (own, near1, near3, across, twice))


def local(
    residual,
    queries,
    key_rows,
    value_rows,
    visible,
    out_proj,
    norm_gain,
    expert_ids,
    route_weight,
    expert_gate,
    expert_up,
    expert_down,
):
    core = lax.axis_index("c")
    first = core == 0
    tokens = residual.shape[0]
    place_x, place_z = lax.axis_index("x"), lax.axis_index("z")
    place_y = 2 * lax.axis_index("h") + lax.axis_index("yl")

    kv_own = jnp.concatenate([half_of(key_rows, core), half_of(value_rows, core)], axis=1)
    kv_give = jnp.concatenate([half_of(key_rows, 1 - core), half_of(value_rows, 1 - core)], axis=1)
    kv_got = crossed(kv_give)
    kv_two = by_core(first, kv_own, kv_got, 0)
    query_got = crossed(half_of(queries, 1 - core))
    query_two = by_core(first, half_of(queries, core), query_got, 0)
    windows = [later(kv_two, blocks) for blocks in (8, 6, 4, 2)] + [kv_two]

    columns = out_proj.shape[1] // 2
    rows_got = moved(out_proj, z=2)
    rows = in_order([out_proj, rows_got], place_z // 2)
    rows_got = crossed(half_of(rows, 1 - core))
    rows = by_core(first, half_of(rows, core), rows_got, 1)
    low, high = rows[..., : columns // 2], rows[..., columns // 2 :]
    low_got = [moved(low, y=step) for step in (1, 2, 3)]
    low = by_height([low, *low_got], place_y)
    low_got = moved(low, x=2)
    low = in_order([low, low_got], place_x // 2).reshape(2, -1, columns // 2)
    high_got = moved(high, x=2)
    high = in_order([high, high_got], place_x // 2)
    high_got = [moved(high, y=step) for step in (1, 2, 3)]
    high = by_height([high, *high_got], place_y).reshape(2, -1, columns // 2)

    chip_block = lax.axis_index(AXES) - core
    seen = lax.dynamic_slice_in_dim(visible, chip_block, 2, 0)
    attended = attend(seen, query_two, windows)
    attended = attended.reshape(4, 2 * tokens, -1)

    ways = ((1, 1), (1, 0), (0, 1), (0, 0))
    same, other = [], []
    for along_x, along_z in ways:
        wanted = (place_x % 2 ^ along_x) * 2 + (place_z % 2 ^ along_z)
        piece = lax.dynamic_index_in_dim(attended, wanted, 0, keepdims=False)
        remote = along_x or along_z
        same.append(to_mate(piece, along_x, along_z, False) if remote else piece)
        other.append(to_mate(piece, along_x, along_z, True) if remote else crossed(piece))
    products = project(core, same, other, low, high)
    straight, switched = [], []
    for place, (along_x, along_z) in enumerate(ways):
        here, there = products[2 * place : 2 * place + 2]
        if along_x or along_z:
            here = from_mate(here, along_x, along_z, False)
            there = from_mate(there, along_x, along_z, True)
        else:
            there = crossed(there)
        straight.append(here.astype(jnp.float32))
        switched.append(there.astype(jnp.float32))
    projected = by_core(first, sum(straight), sum(switched), 1)

    hidden_sum = residual.astype(jnp.float32) + projected
    mean_square = jnp.mean(hidden_sum * hidden_sum, axis=-1, keepdims=True)
    normed = (hidden_sum * lax.rsqrt(mean_square + 1e-05) * norm_gain).astype(jnp.bfloat16)

    mixes, slots = [], []
    for which in range(expert_gate.shape[0]):
        choose = expert_ids == which
        member = jnp.any(choose, axis=1)
        token_weight = jnp.sum(jnp.where(choose, route_weight, 0.0), axis=1)
        ranked = jnp.cumsum(member.astype(jnp.int32)) - member.astype(jnp.int32)
        slot_hit = (ranked[None, :] == jnp.arange(CAP, dtype=jnp.int32)[:, None]) & member[None, :]
        slots.append(slot_hit.astype(jnp.bfloat16))
        mixes.append(jnp.where(slot_hit, token_weight[None, :], 0.0))
    outgoing = jnp.dot(
        jnp.concatenate(slots, axis=0), normed, preferred_element_type=jnp.float32
    ).astype(jnp.bfloat16)

    returned = []
    for which in range(expert_gate.shape[0]):
        pieces = gather_slots(outgoing[which * CAP : (which + 1) * CAP])
        parts = expert(which, pieces, expert_gate, expert_up, expert_down)
        returned.append(return_sums(*parts))
    expert_mix = jnp.dot(
        jnp.concatenate(mixes, axis=0).T,
        jnp.concatenate(returned, axis=0),
        precision=lax.Precision.HIGHEST,
    )
    return (hidden_sum + expert_mix).astype(jnp.bfloat16)


def solution(mesh):
    finer = Mesh(mesh.devices.reshape(SIZES), AXES)
    in_specs = (
        P(AXES, None),
        P(AXES, None),
        P(AXES, None),
        P(AXES, None),
        P(),
        P(AXES, None),
        P(),
        P(AXES, None),
        P(AXES, None),
        P(None, EP, None),
        P(None, EP, None),
        P(None, EP, None),
    )
    return jax.shard_map(
        local, mesh=finer, in_specs=in_specs, out_specs=P(AXES, None), check_vma=False
    )
```

```python
import math

import jax
import jax.numpy as jnp
from jax import lax
from jax.experimental import pallas as pl
from jax.experimental.pallas import tpu as pltpu
from jax.sharding import Mesh
from jax.sharding import PartitionSpec as P


HEAD = 128
CAP = 40
SIZES = (4, 2, 4, 2, 2)
AXES = ("x", "yl", "z", "h", "c")
EP = ("z", "h", "c")


def flat(coords):
    place = 0
    for size, coord in zip(SIZES, coords):
        place = place * size + coord
    return place


def sent(value, rule):
    pairs = []
    for source in range(math.prod(SIZES)):
        rest, coords = source, []
        for size in reversed(SIZES):
            coords.append(rest % size)
            rest //= size
        cx, cyl, cz, ch, cc = reversed(coords)
        x, y, z, core = rule(cx, 2 * ch + cyl, cz, cc)
        pairs.append((source, flat((x % 4, y % 2, z % 4, y % 4 // 2, core))))
    return lax.ppermute(value, AXES, pairs)


def moved(value, x=0, y=0, z=0):
    return sent(value, lambda cx, cy, cz, cc: (cx + x, cy + y, cz + z, cc))


def crossed(value):
    return sent(value, lambda cx, cy, cz, cc: (cx, cy, cz, 1 - cc))


def mate(place, pairing):
    return place + (1 if (place + pairing) % 2 == 0 else -1)


def to_mate(value, along_x, along_z, switch):
    def rule(cx, cy, cz, cc):
        goal = 1 - cc if switch else cc
        return (mate(cx, goal) if along_x else cx, cy, mate(cz, goal) if along_z else cz, goal)

    return sent(value, rule)


def from_mate(value, along_x, along_z, switch):
    def rule(cx, cy, cz, cc):
        goal = 1 - cc if switch else cc
        return (mate(cx, cc) if along_x else cx, cy, mate(cz, cc) if along_z else cz, goal)

    return sent(value, rule)


def later(value, blocks, switch):
    count = math.prod(SIZES)
    return lax.ppermute(
        value, AXES, [(s, (s ^ switch) + blocks) for s in range(count - blocks)]
    )


def half_of(value, which):
    width = value.shape[-1] // 2
    return lax.dynamic_slice_in_dim(value, which * width, width, value.ndim - 1)


def by_core(first, own, other, axis):
    return jnp.where(
        first,
        jnp.concatenate([own, other], axis=axis),
        jnp.concatenate([other, own], axis=axis),
    )


def attend_kernel(core_ref, seen_ref, query_ref, *refs):
    key_refs, value_refs, (out_ref, key_table, value_table) = refs[:10], refs[10:20], refs[20:]
    core = core_ref[0]
    for place in range(10):
        slot = place - place % 2 + (1 - core if place % 2 else core)
        key_table[slot] = key_refs[place][...]
        value_table[slot] = value_refs[place][...]
    keys = key_table[...].reshape(-1, HEAD)
    values = value_table[...].reshape(-1, HEAD)
    factor = math.log2(math.e) / math.sqrt(HEAD)
    tokens = 128
    row = lax.broadcasted_iota(jnp.int32, (tokens, tokens), 0)
    col = lax.broadcasted_iota(jnp.int32, (tokens, tokens), 1)
    causal = jnp.where(col <= row, 0.0, -1e30)
    for block in range(2):
        here = slice(block * tokens, (block + 1) * tokens)
        key_window = keys[block * tokens : (block + 9) * tokens]
        value_window = values[block * tokens : (block + 9) * tokens]
        hidden = [
            jnp.full((tokens, tokens), jnp.where(seen_ref[block, 8 - place] > 0, 0.0, -1e30))
            for place in range(8)
        ]
        bias = jnp.concatenate(hidden + [causal], axis=1)
        query = jnp.concatenate(
            [query_ref[here, head * HEAD : (head + 1) * HEAD] for head in range(4)], axis=0
        )
        scores = lax.dot_general(
            query, key_window, (((1,), (1,)), ((), ())), preferred_element_type=jnp.float32
        )
        weights, totals = [], []
        for head in range(4):
            score = scores[head * tokens : (head + 1) * tokens] + bias
            peak = jnp.max(score, axis=1, keepdims=True)
            weight = jnp.exp2((score - peak) * factor)
            totals.append(jnp.sum(weight, axis=1, keepdims=True))
            weights.append(weight.astype(jnp.bfloat16))
        mixed = jnp.dot(
            jnp.concatenate(weights, axis=0), value_window, preferred_element_type=jnp.float32
        )
        for head in range(4):
            result = mixed[head * tokens : (head + 1) * tokens] / totals[head]
            lanes = slice(head // 2 * HEAD, head // 2 * HEAD + HEAD)
            out_ref[0, head % 2, here, lanes] = result.astype(jnp.bfloat16)


def attend(core, seen, query, windows):
    key_specs = [pl.BlockSpec((128, HEAD), lambda j: (0, j)) for _ in windows]
    value_specs = [pl.BlockSpec((128, HEAD), lambda j: (0, 4 + j)) for _ in windows]
    return pl.pallas_call(
        attend_kernel,
        grid=(4,),
        in_specs=[
            pl.BlockSpec(memory_space=pltpu.SMEM),
            pl.BlockSpec(memory_space=pltpu.SMEM),
            pl.BlockSpec((256, 4 * HEAD), lambda j: (0, j)),
            *key_specs,
            *value_specs,
        ],
        out_specs=pl.BlockSpec((1, 2, 256, 256), lambda j: (j // 2, 0, 0, j % 2)),
        out_shape=jax.ShapeDtypeStruct((2, 2, 256, 512), jnp.bfloat16),
        scratch_shapes=[
            pltpu.VMEM((10, 128, HEAD), jnp.bfloat16),
            pltpu.VMEM((10, 128, HEAD), jnp.bfloat16),
        ],
        name="attend",
        cost_estimate=pl.CostEstimate(
            flops=6_000_000_000, transcendentals=5_000_000, bytes_accessed=6_000_000
        ),
    )(core.reshape(1), seen, query, *windows, *windows)


def in_order(pieces, own_index):
    count = len(pieces)
    table = jnp.zeros((count, *pieces[0].shape), pieces[0].dtype)
    for step, piece in enumerate(pieces):
        table = lax.dynamic_update_index_in_dim(table, piece, (own_index - step) % count, 0)
    return table


def by_height(pieces, place_y):
    shape = pieces[0].shape
    lead = len(shape) - 3
    table = jnp.zeros((*shape[:lead], 2, shape[lead], 2, *shape[lead + 1 :]), pieces[0].dtype)
    for step, piece in enumerate(pieces):
        source = (place_y - step) % 4
        piece = piece.reshape(*shape[:lead], 1, shape[lead], 1, *shape[lead + 1 :])
        start = [0] * table.ndim
        start[lead], start[lead + 2] = source % 2, source // 2
        table = lax.dynamic_update_slice(table, piece, start)
    return table


def project_kernel(core_ref, *refs):
    same, other, row_refs = refs[:8], refs[8:16], refs[16:20]

    def multiply(rows_own, rows_other):
        left = jnp.concatenate([ref[0] for ref in same], axis=0)
        right = jnp.concatenate([ref[0] for ref in other], axis=0)
        product = jnp.dot(left, rows_own[0], preferred_element_type=jnp.float32)
        product += jnp.dot(right, rows_other[0], preferred_element_type=jnp.float32)
        product = product.astype(jnp.bfloat16)
        for place, out_ref in enumerate(refs[20:]):
            out_ref[...] = product[place * 128 : (place + 1) * 128]

    pl.when(pl.program_id(0) < 2)(lambda: multiply(*row_refs[:2]))
    pl.when(pl.program_id(0) >= 2)(lambda: multiply(*row_refs[2:]))


def project(core, same, other, low, high):
    columns = 512
    same = [heads.reshape(2, 128, 512) for heads in same for _ in range(2)]
    other = [heads.reshape(2, 128, 512) for heads in other for _ in range(2)]
    here = pl.BlockSpec((1, 128, 512), lambda n, core: (core[0], 0, 0))
    there = pl.BlockSpec((1, 128, 512), lambda n, core: (1 - core[0], 0, 0))
    out = pl.BlockSpec((128, columns), lambda n, core: (0, n))
    shape = jax.ShapeDtypeStruct((128, 2 * low.shape[2]), jnp.bfloat16)
    early = lambda n: jnp.minimum(n, 1)
    late = lambda n: jnp.maximum(n - 2, 0)
    return pl.pallas_call(
        project_kernel,
        grid_spec=pltpu.PrefetchScalarGridSpec(
            num_scalar_prefetch=1,
            grid=(4,),
            in_specs=[
                *[here, there] * 8,
                pl.BlockSpec((1, 512, columns), lambda n, core: (core[0], 0, early(n))),
                pl.BlockSpec((1, 512, columns), lambda n, core: (1 - core[0], 0, early(n))),
                pl.BlockSpec((1, 512, columns), lambda n, core: (core[0], 0, late(n))),
                pl.BlockSpec((1, 512, columns), lambda n, core: (1 - core[0], 0, late(n))),
            ],
            out_specs=[out] * 8,
        ),
        out_shape=[shape] * 8,
        name="project",
        cost_estimate=pl.CostEstimate(
            flops=4_300_000_000, transcendentals=0, bytes_accessed=10_000_000
        ),
    )(core.reshape(1), *same, *other, low, low, high, high)


def expert_kernel(*refs):
    slot_refs, (gate_ref, up_ref, down_ref, own_ref, other_ref) = refs[:4], refs[4:9]
    gate_sum, up_sum, act = refs[9:]
    step = pl.program_id(0)
    contract = (((1,), (1,)), ((), ()))

    @pl.when(step < 4)
    def _():
        slots = jnp.concatenate([ref[...] for ref in slot_refs], axis=0)
        gate = lax.dot_general(slots, gate_ref[0], contract, preferred_element_type=jnp.float32)
        up = lax.dot_general(slots, up_ref[0], contract, preferred_element_type=jnp.float32)

        @pl.when(step == 0)
        def _():
            gate_sum[...] = gate
            up_sum[...] = up

        @pl.when(step > 0)
        def _():
            gate_sum[...] += gate
            up_sum[...] += up

        @pl.when(step == 3)
        def _():
            value = gate_sum[...]
            act[...] = (value / (1.0 + jnp.exp(-value)) * up_sum[...]).astype(jnp.bfloat16)

    @pl.when(step >= 4)
    def _():
        result = jnp.dot(act[...], down_ref[0], preferred_element_type=jnp.float32)
        result = result.astype(jnp.bfloat16)
        half = result.shape[0] // 2
        own_ref[...] = result[:half]
        other_ref[...] = result[half:]


def expert(which, pieces, gate, up, down):
    slots, width = pieces[0].shape
    hidden = gate.shape[1]
    chunk = width // 4
    rows = len(pieces) * slots
    early = lambda step: jnp.minimum(step, 3)
    late = lambda step: jnp.maximum(step - 4, 0)
    out = pl.BlockSpec((rows // 2, chunk), lambda step: (0, late(step)))
    shape = jax.ShapeDtypeStruct((rows // 2, width), jnp.bfloat16)
    return pl.pallas_call(
        expert_kernel,
        grid=(8,),
        in_specs=[
            *[pl.BlockSpec((slots, chunk), lambda step: (0, early(step))) for _ in pieces],
            pl.BlockSpec((1, hidden, chunk), lambda step: (which, 0, early(step))),
            pl.BlockSpec((1, hidden, chunk), lambda step: (which, 0, early(step))),
            pl.BlockSpec((1, hidden, chunk), lambda step: (which, 0, late(step))),
        ],
        out_specs=[out, out],
        out_shape=[shape, shape],
        scratch_shapes=[
            pltpu.VMEM((rows, hidden), jnp.float32),
            pltpu.VMEM((rows, hidden), jnp.float32),
            pltpu.VMEM((rows, hidden), jnp.bfloat16),
        ],
        name="expert",
        cost_estimate=pl.CostEstimate(
            flops=7_000_000_000, transcendentals=300_000, bytes_accessed=22_000_000
        ),
    )(*pieces, gate, up, down)


def total(*terms):
    return sum(term.astype(jnp.float32) for term in terms).astype(jnp.bfloat16)


def gather_slots(own):
    flip = moved(own, y=2)
    up2, up1, up3 = moved(own, z=2), moved(own, z=1), moved(own, z=3)
    flip1, flip3 = moved(flip, z=1), moved(flip, z=3)
    flip2 = moved(up2, y=2)
    early = jnp.concatenate([own, up1, up3, flip], axis=0)
    late = jnp.concatenate([up2, flip1, flip3, flip2], axis=0)
    early_got = crossed(early)
    late_got = crossed(late)
    return [early, late, early_got, late_got]


def return_sums(own_part, other_part):
    swapped = crossed(other_part)

    def owed(place):
        rows = slice(place * CAP, (place + 1) * CAP)
        return total(own_part[rows], swapped[rows])

    own, up1, up3, flip, up2, flip1, flip3, flip2 = [owed(place) for place in range(8)]
    side1, side3 = moved(flip1, z=3), moved(flip3, z=1)
    far = moved(flip2, y=2)
    near1, near3 = moved(up1, z=3), moved(up3, z=1)
    across = moved(total(flip, side1, side3), y=2)
    twice = moved(total(up2, far), z=2)
    return sum(t.astype(jnp.float32) for t in (own, near1, near3, across, twice))


def local(
    residual,
    queries,
    key_rows,
    value_rows,
    visible,
    out_proj,
    norm_gain,
    expert_ids,
    route_weight,
    expert_gate,
    expert_up,
    expert_down,
):
    core = lax.axis_index("c")
    first = core == 0
    tokens = residual.shape[0]
    place_x, place_z = lax.axis_index("x"), lax.axis_index("z")
    place_y = 2 * lax.axis_index("h") + lax.axis_index("yl")

    kv_own = jnp.concatenate([half_of(key_rows, core), half_of(value_rows, core)], axis=1)
    kv_give = jnp.concatenate([half_of(key_rows, 1 - core), half_of(value_rows, 1 - core)], axis=1)
    kv_got = crossed(kv_give)
    query_got = crossed(half_of(queries, 1 - core))
    query_two = by_core(first, half_of(queries, core), query_got, 0)
    windows = []
    for blocks in (8, 6, 4, 2):
        windows += [later(kv_own, blocks, 0), later(kv_give, blocks, 1)]
    windows += [kv_own, kv_got]

    columns = out_proj.shape[1] // 2
    rows_got = moved(out_proj, z=2)
    rows = in_order([out_proj, rows_got], place_z // 2)
    rows_got = crossed(half_of(rows, 1 - core))
    rows = by_core(first, half_of(rows, core), rows_got, 1)
    rows_got = moved(rows, x=2)
    rows = in_order([rows, rows_got], place_x // 2)
    rows_up, rows_down = moved(rows, y=1), moved(rows, y=3)
    parts = [(piece[..., : columns // 2], piece[..., columns // 2 :]) for piece in (rows, rows_up, rows_down)]
    far_low, far_high = moved(parts[1][0], y=1), moved(parts[2][1], y=3)
    low = by_height([parts[0][0], parts[1][0], far_low, parts[2][0]], place_y)
    high = by_height([parts[0][1], parts[1][1], far_high, parts[2][1]], place_y)
    low, high = low.reshape(2, -1, columns // 2), high.reshape(2, -1, columns // 2)

    chip_block = lax.axis_index(AXES) - core
    seen = lax.dynamic_slice_in_dim(visible, chip_block, 2, 0)
    attended = attend(core, seen, query_two, windows)
    attended = attended.reshape(4, 2 * tokens, -1)

    ways = ((1, 1), (1, 0), (0, 1), (0, 0))
    same, other = [], []
    for along_x, along_z in ways:
        wanted = (place_x % 2 ^ along_x) * 2 + (place_z % 2 ^ along_z)
        piece = lax.dynamic_index_in_dim(attended, wanted, 0, keepdims=False)
        remote = along_x or along_z
        same.append(to_mate(piece, along_x, along_z, False) if remote else piece)
        other.append(to_mate(piece, along_x, along_z, True) if remote else crossed(piece))
    products = project(core, same, other, low, high)
    straight, switched = [], []
    for place, (along_x, along_z) in enumerate(ways):
        here, there = products[2 * place : 2 * place + 2]
        if along_x or along_z:
            here = from_mate(here, along_x, along_z, False)
            there = from_mate(there, along_x, along_z, True)
        else:
            there = crossed(there)
        straight.append(here.astype(jnp.float32))
        switched.append(there.astype(jnp.float32))
    projected = by_core(first, sum(straight), sum(switched), 1)

    hidden_sum = residual.astype(jnp.float32) + projected
    mean_square = jnp.mean(hidden_sum * hidden_sum, axis=-1, keepdims=True)
    normed = (hidden_sum * lax.rsqrt(mean_square + 1e-05) * norm_gain).astype(jnp.bfloat16)

    mixes, slots = [], []
    for which in range(expert_gate.shape[0]):
        choose = expert_ids == which
        member = jnp.any(choose, axis=1)
        token_weight = jnp.sum(jnp.where(choose, route_weight, 0.0), axis=1)
        ranked = jnp.cumsum(member.astype(jnp.int32)) - member.astype(jnp.int32)
        slot_hit = (ranked[None, :] == jnp.arange(CAP, dtype=jnp.int32)[:, None]) & member[None, :]
        slots.append(slot_hit.astype(jnp.bfloat16))
        mixes.append(jnp.where(slot_hit, token_weight[None, :], 0.0))
    outgoing = jnp.dot(
        jnp.concatenate(slots, axis=0), normed, preferred_element_type=jnp.float32
    ).astype(jnp.bfloat16)

    returned = []
    for which in range(expert_gate.shape[0]):
        pieces = gather_slots(outgoing[which * CAP : (which + 1) * CAP])
        parts = expert(which, pieces, expert_gate, expert_up, expert_down)
        returned.append(return_sums(*parts))
    expert_mix = jnp.dot(
        jnp.concatenate(mixes, axis=0).T,
        jnp.concatenate(returned, axis=0),
        precision=lax.Precision.HIGHEST,
    )
    return (hidden_sum + expert_mix).astype(jnp.bfloat16)


def solution(mesh):
    finer = Mesh(mesh.devices.reshape(SIZES), AXES)
    in_specs = (
        P(AXES, None),
        P(AXES, None),
        P(AXES, None),
        P(AXES, None),
        P(),
        P(AXES, None),
        P(),
        P(AXES, None),
        P(AXES, None),
        P(None, EP, None),
        P(None, EP, None),
        P(None, EP, None),
    )
    return jax.shard_map(
        local, mesh=finer, in_specs=in_specs, out_specs=P(AXES, None), check_vma=False
    )
```

```python
import math

import jax
import jax.numpy as jnp
from jax import lax
from jax.experimental import pallas as pl
from jax.experimental.pallas import tpu as pltpu
from jax.sharding import Mesh
from jax.sharding import PartitionSpec as P


HEAD = 128
CAP = 40
SIZES = (4, 2, 4, 2, 2)
AXES = ("x", "yl", "z", "h", "c")
EP = ("z", "h", "c")


def flat(coords):
    place = 0
    for size, coord in zip(SIZES, coords):
        place = place * size + coord
    return place


def sent(value, rule):
    pairs = []
    for source in range(math.prod(SIZES)):
        rest, coords = source, []
        for size in reversed(SIZES):
            coords.append(rest % size)
            rest //= size
        cx, cyl, cz, ch, cc = reversed(coords)
        x, y, z, core = rule(cx, 2 * ch + cyl, cz, cc)
        pairs.append((source, flat((x % 4, y % 2, z % 4, y % 4 // 2, core))))
    return lax.ppermute(value, AXES, pairs)


def moved(value, x=0, y=0, z=0):
    return sent(value, lambda cx, cy, cz, cc: (cx + x, cy + y, cz + z, cc))


def crossed(value):
    return sent(value, lambda cx, cy, cz, cc: (cx, cy, cz, 1 - cc))


def mate(place, pairing):
    return place + (1 if (place + pairing) % 2 == 0 else -1)


def to_mate(value, along_x, along_z, switch):
    def rule(cx, cy, cz, cc):
        goal = 1 - cc if switch else cc
        return (mate(cx, goal) if along_x else cx, cy, mate(cz, goal) if along_z else cz, goal)

    return sent(value, rule)


def from_mate(value, along_x, along_z, switch):
    def rule(cx, cy, cz, cc):
        goal = 1 - cc if switch else cc
        return (mate(cx, cc) if along_x else cx, cy, mate(cz, cc) if along_z else cz, goal)

    return sent(value, rule)


def later(value, blocks, switch):
    count = math.prod(SIZES)
    return lax.ppermute(
        value, AXES, [(s, (s ^ switch) + blocks) for s in range(count - blocks)]
    )


def half_of(value, which):
    width = value.shape[-1] // 2
    return lax.dynamic_slice_in_dim(value, which * width, width, value.ndim - 1)


def by_core(first, own, other, axis):
    return jnp.where(
        first,
        jnp.concatenate([own, other], axis=axis),
        jnp.concatenate([other, own], axis=axis),
    )


def attend_kernel(core_ref, seen_ref, query_ref, *refs):
    key_refs, value_refs, (out_ref, key_table, value_table) = refs[:10], refs[10:20], refs[20:]
    core = core_ref[0]
    for place in range(10):
        slot = place - place % 2 + (1 - core if place % 2 else core)
        key_table[slot] = key_refs[place][...]
        value_table[slot] = value_refs[place][...]
    keys = key_table[...].reshape(-1, HEAD)
    values = value_table[...].reshape(-1, HEAD)
    factor = math.log2(math.e) / math.sqrt(HEAD)
    tokens = 128
    row = lax.broadcasted_iota(jnp.int32, (tokens, tokens), 0)
    col = lax.broadcasted_iota(jnp.int32, (tokens, tokens), 1)
    causal = jnp.where(col <= row, 0.0, -1e30)
    for block in range(2):
        here = slice(block * tokens, (block + 1) * tokens)
        key_window = keys[block * tokens : (block + 9) * tokens]
        value_window = values[block * tokens : (block + 9) * tokens]
        hidden = [
            jnp.full((tokens, tokens), jnp.where(seen_ref[block, 8 - place] > 0, 0.0, -1e30))
            for place in range(8)
        ]
        bias = jnp.concatenate(hidden + [causal], axis=1)
        query = jnp.concatenate(
            [query_ref[here, head * HEAD : (head + 1) * HEAD] for head in range(4)], axis=0
        )
        scores = lax.dot_general(
            query, key_window, (((1,), (1,)), ((), ())), preferred_element_type=jnp.float32
        )
        weights, totals = [], []
        for head in range(4):
            score = scores[head * tokens : (head + 1) * tokens] + bias
            peak = jnp.max(score, axis=1, keepdims=True)
            weight = jnp.exp2((score - peak) * factor)
            totals.append(jnp.sum(weight, axis=1, keepdims=True))
            weights.append(weight.astype(jnp.bfloat16))
        mixed = jnp.dot(
            jnp.concatenate(weights, axis=0), value_window, preferred_element_type=jnp.float32
        )
        for head in range(4):
            result = mixed[head * tokens : (head + 1) * tokens] / totals[head]
            lanes = slice(head // 2 * HEAD, head // 2 * HEAD + HEAD)
            out_ref[0, head % 2, here, lanes] = result.astype(jnp.bfloat16)


def attend(core, seen, query, windows):
    key_specs = [pl.BlockSpec((128, HEAD), lambda j: (0, j)) for _ in windows]
    value_specs = [pl.BlockSpec((128, HEAD), lambda j: (0, 4 + j)) for _ in windows]
    return pl.pallas_call(
        attend_kernel,
        grid=(4,),
        in_specs=[
            pl.BlockSpec(memory_space=pltpu.SMEM),
            pl.BlockSpec(memory_space=pltpu.SMEM),
            pl.BlockSpec((256, 4 * HEAD), lambda j: (0, j)),
            *key_specs,
            *value_specs,
        ],
        out_specs=pl.BlockSpec((1, 2, 256, 256), lambda j: (j // 2, 0, 0, j % 2)),
        out_shape=jax.ShapeDtypeStruct((2, 2, 256, 512), jnp.bfloat16),
        scratch_shapes=[
            pltpu.VMEM((10, 128, HEAD), jnp.bfloat16),
            pltpu.VMEM((10, 128, HEAD), jnp.bfloat16),
        ],
        name="attend",
        cost_estimate=pl.CostEstimate(
            flops=6_000_000_000, transcendentals=5_000_000, bytes_accessed=6_000_000
        ),
    )(core.reshape(1), seen, query, *windows, *windows)


def in_order(pieces, own_index):
    count = len(pieces)
    table = jnp.zeros((count, *pieces[0].shape), pieces[0].dtype)
    for step, piece in enumerate(pieces):
        table = lax.dynamic_update_index_in_dim(table, piece, (own_index - step) % count, 0)
    return table


def by_height(pieces, place_y):
    shape = pieces[0].shape
    lead = len(shape) - 3
    table = jnp.zeros((*shape[:lead], 2, shape[lead], 2, *shape[lead + 1 :]), pieces[0].dtype)
    for step, piece in enumerate(pieces):
        source = (place_y - step) % 4
        piece = piece.reshape(*shape[:lead], 1, shape[lead], 1, *shape[lead + 1 :])
        start = [0] * table.ndim
        start[lead], start[lead + 2] = source % 2, source // 2
        table = lax.dynamic_update_slice(table, piece, start)
    return table


def project_kernel(core_ref, *refs):
    same, other, row_refs = refs[:8], refs[8:16], refs[16:20]

    def multiply(rows_own, rows_other):
        left = jnp.concatenate([ref[0] for ref in same], axis=0)
        right = jnp.concatenate([ref[0] for ref in other], axis=0)
        product = jnp.dot(left, rows_own[0], preferred_element_type=jnp.float32)
        product += jnp.dot(right, rows_other[0], preferred_element_type=jnp.float32)
        product = product.astype(jnp.bfloat16)
        for place, out_ref in enumerate(refs[20:]):
            out_ref[...] = product[place * 128 : (place + 1) * 128]

    pl.when(pl.program_id(0) < 2)(lambda: multiply(*row_refs[:2]))
    pl.when(pl.program_id(0) >= 2)(lambda: multiply(*row_refs[2:]))


def project(core, same, other, low, high):
    columns = 512
    same = [heads.reshape(2, 128, 512) for heads in same for _ in range(2)]
    other = [heads.reshape(2, 128, 512) for heads in other for _ in range(2)]
    here = pl.BlockSpec((1, 128, 512), lambda n, core: (core[0], 0, 0))
    there = pl.BlockSpec((1, 128, 512), lambda n, core: (1 - core[0], 0, 0))
    out = pl.BlockSpec((128, columns), lambda n, core: (0, n))
    shape = jax.ShapeDtypeStruct((128, 2 * low.shape[2]), jnp.bfloat16)
    early = lambda n: jnp.minimum(n, 1)
    late = lambda n: jnp.maximum(n - 2, 0)
    return pl.pallas_call(
        project_kernel,
        grid_spec=pltpu.PrefetchScalarGridSpec(
            num_scalar_prefetch=1,
            grid=(4,),
            in_specs=[
                *[here, there] * 8,
                pl.BlockSpec((1, 512, columns), lambda n, core: (core[0], 0, early(n))),
                pl.BlockSpec((1, 512, columns), lambda n, core: (1 - core[0], 0, early(n))),
                pl.BlockSpec((1, 512, columns), lambda n, core: (core[0], 0, late(n))),
                pl.BlockSpec((1, 512, columns), lambda n, core: (1 - core[0], 0, late(n))),
            ],
            out_specs=[out] * 8,
        ),
        out_shape=[shape] * 8,
        name="project",
        cost_estimate=pl.CostEstimate(
            flops=4_300_000_000, transcendentals=0, bytes_accessed=10_000_000
        ),
    )(core.reshape(1), *same, *other, low, low, high, high)


def expert_kernel(*refs):
    slot_refs, (gate_ref, up_ref, down_ref, own_ref, other_ref) = refs[:4], refs[4:9]
    gate_sum, up_sum, act = refs[9:]
    step = pl.program_id(0)
    contract = (((1,), (1,)), ((), ()))

    @pl.when(step == 0)
    def _():
        gate_sum[...] = jnp.zeros_like(gate_sum)
        up_sum[...] = jnp.zeros_like(up_sum)

    @pl.when(step < 2)
    def _():
        slots = jnp.concatenate([ref[...] for ref in slot_refs], axis=0)
        gate = lax.dot_general(slots, gate_ref[0], contract, preferred_element_type=jnp.float32)
        up = lax.dot_general(slots, up_ref[0], contract, preferred_element_type=jnp.float32)
        gate_sum[...] += gate
        up_sum[...] += up

        @pl.when(step == 1)
        def _():
            value = gate_sum[...]
            act[...] = (value / (1.0 + jnp.exp(-value)) * up_sum[...]).astype(jnp.bfloat16)

    @pl.when(step >= 2)
    def _():
        result = jnp.dot(act[...], down_ref[0], preferred_element_type=jnp.float32)
        result = result.astype(jnp.bfloat16)
        half = result.shape[0] // 2
        own_ref[...] = result[:half]
        other_ref[...] = result[half:]


def expert(which, pieces, gate, up, down):
    slots, width = pieces[0].shape
    hidden = gate.shape[1]
    chunk = width // 2
    rows = len(pieces) * slots
    early = lambda step: jnp.minimum(step, 1)
    late = lambda step: jnp.maximum(step - 2, 0)
    out = pl.BlockSpec((rows // 2, chunk), lambda step: (0, late(step)))
    shape = jax.ShapeDtypeStruct((rows // 2, width), jnp.bfloat16)
    return pl.pallas_call(
        expert_kernel,
        grid=(4,),
        in_specs=[
            *[pl.BlockSpec((slots, chunk), lambda step: (0, early(step))) for _ in pieces],
            pl.BlockSpec((1, hidden, chunk), lambda step: (which, 0, early(step))),
            pl.BlockSpec((1, hidden, chunk), lambda step: (which, 0, early(step))),
            pl.BlockSpec((1, hidden, chunk), lambda step: (which, 0, late(step))),
        ],
        out_specs=[out, out],
        out_shape=[shape, shape],
        scratch_shapes=[
            pltpu.VMEM((rows, hidden), jnp.float32),
            pltpu.VMEM((rows, hidden), jnp.float32),
            pltpu.VMEM((rows, hidden), jnp.bfloat16),
        ],
        name="expert",
        cost_estimate=pl.CostEstimate(
            flops=7_000_000_000, transcendentals=300_000, bytes_accessed=22_000_000
        ),
    )(*pieces, gate, up, down)


def total(*terms):
    return sum(term.astype(jnp.float32) for term in terms).astype(jnp.bfloat16)


def gather_slots(own):
    flip = moved(own, y=2)
    far = moved(own, z=2)
    flip_far = moved(far, y=2)
    both = jnp.concatenate([own, flip], axis=0)
    ring1, ring3 = moved(both, z=1), moved(both, z=3)
    early = jnp.concatenate([both, far, flip_far], axis=0)
    early_got = crossed(early)
    late = jnp.concatenate([ring1, ring3], axis=0)
    late_got = crossed(late)
    return [early, late, early_got, late_got]


def return_sums(own_part, other_part):
    swapped = crossed(other_part)

    def owed(place, count=1):
        rows = slice(place * CAP, (place + count) * CAP)
        return total(own_part[rows], swapped[rows])

    here, flip, far, flip_far, ring1, ring3 = lax.optimization_barrier(
        (owed(0), owed(1), owed(2), owed(3), owed(4, 2), owed(6, 2))
    )
    flip_far = moved(flip_far, y=2)
    ring1, ring3 = moved(ring1, z=3), moved(ring3, z=1)
    across = moved(total(flip, ring1[CAP:], ring3[CAP:]), y=2)
    twice = moved(total(far, flip_far), z=2)
    return sum(t.astype(jnp.float32) for t in (here, ring1[:CAP], ring3[:CAP], across, twice))


def local(
    residual,
    queries,
    key_rows,
    value_rows,
    visible,
    out_proj,
    norm_gain,
    expert_ids,
    route_weight,
    expert_gate,
    expert_up,
    expert_down,
):
    core = lax.axis_index("c")
    first = core == 0
    tokens = residual.shape[0]
    place_x, place_z = lax.axis_index("x"), lax.axis_index("z")
    place_y = 2 * lax.axis_index("h") + lax.axis_index("yl")

    kv_own = jnp.concatenate([half_of(key_rows, core), half_of(value_rows, core)], axis=1)
    kv_give = jnp.concatenate([half_of(key_rows, 1 - core), half_of(value_rows, 1 - core)], axis=1)
    kv_got = crossed(kv_give)
    query_got = crossed(half_of(queries, 1 - core))
    query_two = by_core(first, half_of(queries, core), query_got, 0)
    windows = []
    for blocks in (8, 6, 4, 2):
        windows += [later(kv_own, blocks, 0), later(kv_give, blocks, 1)]
    windows += [kv_own, kv_got]

    columns = out_proj.shape[1] // 2
    rows_got = moved(out_proj, z=2)
    rows = in_order([out_proj, rows_got], place_z // 2)
    rows_got = crossed(half_of(rows, 1 - core))
    rows = by_core(first, half_of(rows, core), rows_got, 1)
    rows_got = moved(rows, x=2)
    rows = in_order([rows, rows_got], place_x // 2)
    rows_up, rows_down = moved(rows, y=1), moved(rows, y=3)
    parts = [(piece[..., : columns // 2], piece[..., columns // 2 :]) for piece in (rows, rows_up, rows_down)]
    far_low, far_high = moved(parts[1][0], y=1), moved(parts[2][1], y=3)
    low = by_height([parts[0][0], parts[1][0], far_low, parts[2][0]], place_y)
    high = by_height([parts[0][1], parts[1][1], far_high, parts[2][1]], place_y)
    low, high = low.reshape(2, -1, columns // 2), high.reshape(2, -1, columns // 2)

    chip_block = lax.axis_index(AXES) - core
    seen = lax.dynamic_slice_in_dim(visible, chip_block, 2, 0)
    attended = attend(core, seen, query_two, windows)
    attended = attended.reshape(4, 2 * tokens, -1)

    ways = ((1, 1), (1, 0), (0, 1), (0, 0))
    same, other = [], []
    for along_x, along_z in ways:
        wanted = (place_x % 2 ^ along_x) * 2 + (place_z % 2 ^ along_z)
        piece = lax.dynamic_index_in_dim(attended, wanted, 0, keepdims=False)
        remote = along_x or along_z
        same.append(to_mate(piece, along_x, along_z, False) if remote else piece)
        other.append(to_mate(piece, along_x, along_z, True) if remote else crossed(piece))
    products = project(core, same, other, low, high)
    straight, switched = [], []
    for place, (along_x, along_z) in enumerate(ways):
        here, there = products[2 * place : 2 * place + 2]
        if along_x or along_z:
            here = from_mate(here, along_x, along_z, False)
            there = from_mate(there, along_x, along_z, True)
        else:
            there = crossed(there)
        straight.append(here.astype(jnp.float32))
        switched.append(there.astype(jnp.float32))
    projected = by_core(first, sum(straight), sum(switched), 1)

    hidden_sum = residual.astype(jnp.float32) + projected
    mean_square = jnp.mean(hidden_sum * hidden_sum, axis=-1, keepdims=True)
    normed = (hidden_sum * lax.rsqrt(mean_square + 1e-05) * norm_gain).astype(jnp.bfloat16)

    mixes, slots = [], []
    for which in range(expert_gate.shape[0]):
        choose = expert_ids == which
        member = jnp.any(choose, axis=1)
        token_weight = jnp.sum(jnp.where(choose, route_weight, 0.0), axis=1)
        ranked = jnp.cumsum(member.astype(jnp.int32)) - member.astype(jnp.int32)
        slot_hit = (ranked[None, :] == jnp.arange(CAP, dtype=jnp.int32)[:, None]) & member[None, :]
        slots.append(slot_hit.astype(jnp.bfloat16))
        mixes.append(jnp.where(slot_hit, token_weight[None, :], 0.0))
    outgoing = jnp.dot(
        jnp.concatenate(slots, axis=0), normed, preferred_element_type=jnp.float32
    ).astype(jnp.bfloat16)

    returned = []
    for which in range(expert_gate.shape[0]):
        pieces = gather_slots(outgoing[which * CAP : (which + 1) * CAP])
        parts = expert(which, pieces, expert_gate, expert_up, expert_down)
        returned.append(return_sums(*parts))
    expert_mix = jnp.dot(
        jnp.concatenate(mixes, axis=0).T,
        jnp.concatenate(returned, axis=0),
        precision=lax.Precision.HIGHEST,
    )
    return (hidden_sum + expert_mix).astype(jnp.bfloat16)


def solution(mesh):
    finer = Mesh(mesh.devices.reshape(SIZES), AXES)
    in_specs = (
        P(AXES, None),
        P(AXES, None),
        P(AXES, None),
        P(AXES, None),
        P(),
        P(AXES, None),
        P(),
        P(AXES, None),
        P(AXES, None),
        P(None, EP, None),
        P(None, EP, None),
        P(None, EP, None),
    )
    return jax.shard_map(
        local, mesh=finer, in_specs=in_specs, out_specs=P(AXES, None), check_vma=False
    )
```

```python
import math

import jax
import jax.numpy as jnp
from jax import lax
from jax.experimental import pallas as pl
from jax.experimental.pallas import tpu as pltpu
from jax.sharding import Mesh
from jax.sharding import PartitionSpec as P


HEAD = 128
CAP = 40
SIZES = (4, 2, 4, 2, 2)
AXES = ("x", "yl", "z", "h", "c")
EP = ("z", "h", "c")


def flat(coords):
    place = 0
    for size, coord in zip(SIZES, coords):
        place = place * size + coord
    return place


def sent(value, rule):
    pairs = []
    for source in range(math.prod(SIZES)):
        rest, coords = source, []
        for size in reversed(SIZES):
            coords.append(rest % size)
            rest //= size
        cx, cyl, cz, ch, cc = reversed(coords)
        x, y, z, core = rule(cx, 2 * ch + cyl, cz, cc)
        pairs.append((source, flat((x % 4, y % 2, z % 4, y % 4 // 2, core))))
    return lax.ppermute(value, AXES, pairs)


def moved(value, x=0, y=0, z=0):
    return sent(value, lambda cx, cy, cz, cc: (cx + x, cy + y, cz + z, cc))


def crossed(value):
    return sent(value, lambda cx, cy, cz, cc: (cx, cy, cz, 1 - cc))


def mate(place, pairing):
    return place + (1 if (place + pairing) % 2 == 0 else -1)


def to_mate(value, along_x, along_z, switch):
    def rule(cx, cy, cz, cc):
        goal = 1 - cc if switch else cc
        return (mate(cx, goal) if along_x else cx, cy, mate(cz, goal) if along_z else cz, goal)

    return sent(value, rule)


def from_mate(value, along_x, along_z, switch):
    def rule(cx, cy, cz, cc):
        goal = 1 - cc if switch else cc
        return (mate(cx, cc) if along_x else cx, cy, mate(cz, cc) if along_z else cz, goal)

    return sent(value, rule)


def later(value, blocks, switch):
    count = math.prod(SIZES)
    return lax.ppermute(
        value, AXES, [(s, (s ^ switch) + blocks) for s in range(count - blocks)]
    )


def half_of(value, which):
    width = value.shape[-1] // 2
    return lax.dynamic_slice_in_dim(value, which * width, width, value.ndim - 1)


def by_core(first, own, other, axis):
    return jnp.where(
        first,
        jnp.concatenate([own, other], axis=axis),
        jnp.concatenate([other, own], axis=axis),
    )


def attend_kernel(core_ref, seen_ref, query_ref, *refs):
    key_refs, value_refs, (out_ref, key_table, value_table) = refs[:10], refs[10:20], refs[20:]
    core = core_ref[0]
    for place in range(10):
        slot = place - place % 2 + (1 - core if place % 2 else core)
        key_table[slot] = key_refs[place][...]
        value_table[slot] = value_refs[place][...]
    factor = math.log2(math.e) / math.sqrt(HEAD)
    tokens = 128
    row = lax.broadcasted_iota(jnp.int32, (tokens, tokens), 0)
    col = lax.broadcasted_iota(jnp.int32, (tokens, tokens), 1)
    causal = jnp.where(col <= row, 0.0, -1e30)

    @pl.loop(0, 2)
    def _(block):
        here = pl.ds(pl.multiple_of(block * tokens, tokens), tokens)
        key_window = key_table[pl.ds(block, 9)].reshape(-1, HEAD)
        value_window = value_table[pl.ds(block, 9)].reshape(-1, HEAD)
        hidden = [
            jnp.full((tokens, tokens), jnp.where(seen_ref[block, 8 - place] > 0, 0.0, -1e30))
            for place in range(8)
        ]
        bias = jnp.concatenate(hidden + [causal], axis=1)
        query = jnp.concatenate(
            [query_ref[here, head * HEAD : (head + 1) * HEAD] for head in range(4)], axis=0
        )
        scores = lax.dot_general(
            query, key_window, (((1,), (1,)), ((), ())), preferred_element_type=jnp.float32
        )
        weights, totals = [], []
        for head in range(4):
            score = scores[head * tokens : (head + 1) * tokens] + bias
            peak = jnp.max(score, axis=1, keepdims=True)
            weight = jnp.exp2((score - peak) * factor)
            totals.append(jnp.sum(weight, axis=1, keepdims=True))
            weights.append(weight.astype(jnp.bfloat16))
        mixed = jnp.dot(
            jnp.concatenate(weights, axis=0), value_window, preferred_element_type=jnp.float32
        )
        for head in range(4):
            result = mixed[head * tokens : (head + 1) * tokens] / totals[head]
            lanes = slice(head // 2 * HEAD, head // 2 * HEAD + HEAD)
            out_ref[0, head % 2, here, lanes] = result.astype(jnp.bfloat16)


def attend(core, seen, query, windows):
    key_specs = [pl.BlockSpec((128, HEAD), lambda j: (0, j)) for _ in windows]
    value_specs = [pl.BlockSpec((128, HEAD), lambda j: (0, 4 + j)) for _ in windows]
    return pl.pallas_call(
        attend_kernel,
        grid=(4,),
        in_specs=[
            pl.BlockSpec(memory_space=pltpu.SMEM),
            pl.BlockSpec(memory_space=pltpu.SMEM),
            pl.BlockSpec((256, 4 * HEAD), lambda j: (0, j)),
            *key_specs,
            *value_specs,
        ],
        out_specs=pl.BlockSpec((1, 2, 256, 256), lambda j: (j // 2, 0, 0, j % 2)),
        out_shape=jax.ShapeDtypeStruct((2, 2, 256, 512), jnp.bfloat16),
        scratch_shapes=[
            pltpu.VMEM((10, 128, HEAD), jnp.bfloat16),
            pltpu.VMEM((10, 128, HEAD), jnp.bfloat16),
        ],
        name="attend",
        cost_estimate=pl.CostEstimate(
            flops=6_000_000_000, transcendentals=5_000_000, bytes_accessed=6_000_000
        ),
    )(core.reshape(1), seen, query, *windows, *windows)


def in_order(pieces, own_index):
    count = len(pieces)
    table = jnp.zeros((count, *pieces[0].shape), pieces[0].dtype)
    for step, piece in enumerate(pieces):
        table = lax.dynamic_update_index_in_dim(table, piece, (own_index - step) % count, 0)
    return table


def by_height(pieces, place_y):
    x_half, z_half, rows, columns = pieces[0][2].shape
    table = jnp.zeros((x_half, 2, z_half, 2, rows, columns), pieces[0][2].dtype)
    for step, column, piece in pieces:
        source = (place_y - step) % 4
        piece = piece.reshape(x_half, 1, z_half, 1, rows, -1)
        table = lax.dynamic_update_slice(table, piece, (0, source % 2, 0, source // 2, 0, column))
    return table


def project_kernel(core_ref, *refs):
    same, other, (rows_own, rows_other) = refs[:8], refs[8:16], refs[16:18]
    left = jnp.concatenate([ref[0] for ref in same], axis=0)
    right = jnp.concatenate([ref[0] for ref in other], axis=0)
    product = jnp.dot(left, rows_own[0], preferred_element_type=jnp.float32)
    product += jnp.dot(right, rows_other[0], preferred_element_type=jnp.float32)
    product = product.astype(jnp.bfloat16)
    for place, out_ref in enumerate(refs[18:]):
        out_ref[...] = product[place * 128 : (place + 1) * 128]


def project(core, same, other, rows):
    columns = 512
    same = [heads.reshape(2, 128, 512) for heads in same for _ in range(2)]
    other = [heads.reshape(2, 128, 512) for heads in other for _ in range(2)]
    here = pl.BlockSpec((1, 128, 512), lambda n, core: (core[0], 0, 0))
    there = pl.BlockSpec((1, 128, 512), lambda n, core: (1 - core[0], 0, 0))
    out = pl.BlockSpec((128, columns), lambda n, core: (0, n))
    shape = jax.ShapeDtypeStruct((128, rows.shape[2]), jnp.bfloat16)
    return pl.pallas_call(
        project_kernel,
        grid_spec=pltpu.PrefetchScalarGridSpec(
            num_scalar_prefetch=1,
            grid=(4,),
            in_specs=[
                *[here, there] * 8,
                pl.BlockSpec((1, 512, columns), lambda n, core: (core[0], 0, n)),
                pl.BlockSpec((1, 512, columns), lambda n, core: (1 - core[0], 0, n)),
            ],
            out_specs=[out] * 8,
        ),
        out_shape=[shape] * 8,
        name="project",
        cost_estimate=pl.CostEstimate(
            flops=4_300_000_000, transcendentals=0, bytes_accessed=10_000_000
        ),
    )(core.reshape(1), *same, *other, rows, rows)


def expert_kernel(*refs):
    slot_refs, (gate_ref, up_ref, down_ref, own_ref, other_ref) = refs[:4], refs[4:9]
    gate_sum, up_sum, act = refs[9:]
    step = pl.program_id(0)
    contract = (((1,), (1,)), ((), ()))

    @pl.when(step == 0)
    def _():
        gate_sum[...] = jnp.zeros_like(gate_sum)
        up_sum[...] = jnp.zeros_like(up_sum)

    @pl.when(step < 2)
    def _():
        slots = jnp.concatenate([ref[...] for ref in slot_refs], axis=0)
        gate = lax.dot_general(slots, gate_ref[0], contract, preferred_element_type=jnp.float32)
        up = lax.dot_general(slots, up_ref[0], contract, preferred_element_type=jnp.float32)
        gate_sum[...] += gate
        up_sum[...] += up

        @pl.when(step == 1)
        def _():
            value = gate_sum[...]
            act[...] = (value / (1.0 + jnp.exp(-value)) * up_sum[...]).astype(jnp.bfloat16)

    @pl.when(step >= 2)
    def _():
        result = jnp.dot(act[...], down_ref[0], preferred_element_type=jnp.float32)
        result = result.astype(jnp.bfloat16)
        half = result.shape[0] // 2
        own_ref[...] = result[:half]
        other_ref[...] = result[half:]


def expert(which, pieces, gate, up, down):
    slots, width = pieces[0].shape
    hidden = gate.shape[1]
    chunk = width // 2
    rows = len(pieces) * slots
    early = lambda step: jnp.minimum(step, 1)
    late = lambda step: jnp.maximum(step - 2, 0)
    out = pl.BlockSpec((rows // 2, chunk), lambda step: (0, late(step)))
    shape = jax.ShapeDtypeStruct((rows // 2, width), jnp.bfloat16)
    return pl.pallas_call(
        expert_kernel,
        grid=(4,),
        in_specs=[
            *[pl.BlockSpec((slots, chunk), lambda step: (0, early(step))) for _ in pieces],
            pl.BlockSpec((1, hidden, chunk), lambda step: (which, 0, early(step))),
            pl.BlockSpec((1, hidden, chunk), lambda step: (which, 0, early(step))),
            pl.BlockSpec((1, hidden, chunk), lambda step: (which, 0, late(step))),
        ],
        out_specs=[out, out],
        out_shape=[shape, shape],
        scratch_shapes=[
            pltpu.VMEM((rows, hidden), jnp.float32),
            pltpu.VMEM((rows, hidden), jnp.float32),
            pltpu.VMEM((rows, hidden), jnp.bfloat16),
        ],
        name="expert",
        cost_estimate=pl.CostEstimate(
            flops=7_000_000_000, transcendentals=300_000, bytes_accessed=22_000_000
        ),
    )(*pieces, gate, up, down)


def total(*terms):
    return sum(term.astype(jnp.float32) for term in terms).astype(jnp.bfloat16)


def gather_slots(own):
    flip = moved(own, y=2)
    far = moved(own, z=2)
    flip_far = moved(far, y=2)
    both = jnp.concatenate([own, flip], axis=0)
    ring1, ring3 = moved(both, z=1), moved(both, z=3)
    early = jnp.concatenate([both, far, flip_far], axis=0)
    early_got = crossed(early)
    late = jnp.concatenate([ring1, ring3], axis=0)
    late_got = crossed(late)
    return [early, late, early_got, late_got]


def return_sums(own_part, other_part):
    swapped = crossed(other_part)

    def owed(place, count=1):
        rows = slice(place * CAP, (place + count) * CAP)
        return total(own_part[rows], swapped[rows])

    here, flip, far, flip_far, ring1, ring3 = lax.optimization_barrier(
        (owed(0), owed(1), owed(2), owed(3), owed(4, 2), owed(6, 2))
    )
    flip_far = moved(flip_far, y=2)
    ring1, ring3 = moved(ring1, z=3), moved(ring3, z=1)
    across = moved(total(flip, ring1[CAP:], ring3[CAP:]), y=2)
    twice = moved(total(far, flip_far), z=2)
    return sum(t.astype(jnp.float32) for t in (here, ring1[:CAP], ring3[:CAP], across, twice))


def local(
    residual,
    queries,
    key_rows,
    value_rows,
    visible,
    out_proj,
    norm_gain,
    expert_ids,
    route_weight,
    expert_gate,
    expert_up,
    expert_down,
):
    core = lax.axis_index("c")
    first = core == 0
    tokens = residual.shape[0]
    place_x, place_z = lax.axis_index("x"), lax.axis_index("z")
    place_y = 2 * lax.axis_index("h") + lax.axis_index("yl")

    kv_own = jnp.concatenate([half_of(key_rows, core), half_of(value_rows, core)], axis=1)
    kv_give = jnp.concatenate([half_of(key_rows, 1 - core), half_of(value_rows, 1 - core)], axis=1)
    kv_got = crossed(kv_give)
    query_got = crossed(half_of(queries, 1 - core))
    query_two = by_core(first, half_of(queries, core), query_got, 0)
    windows = []
    for blocks in (8, 6, 4, 2):
        windows += [later(kv_own, blocks, 0), later(kv_give, blocks, 1)]
    windows += [kv_own, kv_got]

    columns = out_proj.shape[1] // 2
    rows_got = moved(out_proj, z=2)
    rows = in_order([out_proj, rows_got], place_z // 2)
    rows_got = crossed(half_of(rows, 1 - core))
    rows = by_core(first, half_of(rows, core), rows_got, 1)
    rows_got = moved(rows, x=2)
    rows = in_order([rows, rows_got], place_x // 2)
    rows_up, rows_down = moved(rows, y=1), moved(rows, y=3)
    half = columns // 2
    far_low, far_high = moved(rows_up[..., :half], y=1), moved(rows_down[..., half:], y=3)
    pieces = [(0, 0, rows), (1, 0, rows_up), (3, 0, rows_down), (2, 0, far_low), (2, half, far_high)]
    rows = by_height(pieces, place_y).reshape(2, -1, columns)

    chip_block = lax.axis_index(AXES) - core
    seen = lax.dynamic_slice_in_dim(visible, chip_block, 2, 0)
    attended = attend(core, seen, query_two, windows)
    attended = attended.reshape(4, 2 * tokens, -1)

    ways = ((1, 1), (1, 0), (0, 1), (0, 0))
    same, other = [], []
    for along_x, along_z in ways:
        wanted = (place_x % 2 ^ along_x) * 2 + (place_z % 2 ^ along_z)
        piece = lax.dynamic_index_in_dim(attended, wanted, 0, keepdims=False)
        remote = along_x or along_z
        same.append(to_mate(piece, along_x, along_z, False) if remote else piece)
        other.append(to_mate(piece, along_x, along_z, True) if remote else crossed(piece))
    products = project(core, same, other, rows)
    straight, switched = [], []
    for place, (along_x, along_z) in enumerate(ways):
        here, there = products[2 * place : 2 * place + 2]
        if along_x or along_z:
            here = from_mate(here, along_x, along_z, False)
            there = from_mate(there, along_x, along_z, True)
        else:
            there = crossed(there)
        straight.append(here.astype(jnp.float32))
        switched.append(there.astype(jnp.float32))
    projected = by_core(first, sum(straight), sum(switched), 1)

    hidden_sum = residual.astype(jnp.float32) + projected
    mean_square = jnp.mean(hidden_sum * hidden_sum, axis=-1, keepdims=True)
    normed = (hidden_sum * lax.rsqrt(mean_square + 1e-05) * norm_gain).astype(jnp.bfloat16)

    mixes, slots = [], []
    for which in range(expert_gate.shape[0]):
        choose = expert_ids == which
        member = jnp.any(choose, axis=1)
        token_weight = jnp.sum(jnp.where(choose, route_weight, 0.0), axis=1)
        ranked = jnp.cumsum(member.astype(jnp.int32)) - member.astype(jnp.int32)
        slot_hit = (ranked[None, :] == jnp.arange(CAP, dtype=jnp.int32)[:, None]) & member[None, :]
        slots.append(slot_hit.astype(jnp.bfloat16))
        mixes.append(jnp.where(slot_hit, token_weight[None, :], 0.0))
    outgoing = jnp.dot(
        jnp.concatenate(slots, axis=0), normed, preferred_element_type=jnp.float32
    ).astype(jnp.bfloat16)

    returned = []
    for which in range(expert_gate.shape[0]):
        pieces = gather_slots(outgoing[which * CAP : (which + 1) * CAP])
        parts = expert(which, pieces, expert_gate, expert_up, expert_down)
        returned.append(return_sums(*parts))
    expert_mix = jnp.dot(
        jnp.concatenate(mixes, axis=0).T,
        jnp.concatenate(returned, axis=0),
        precision=lax.Precision.HIGHEST,
    )
    return (hidden_sum + expert_mix).astype(jnp.bfloat16)


def solution(mesh):
    finer = Mesh(mesh.devices.reshape(SIZES), AXES)
    in_specs = (
        P(AXES, None),
        P(AXES, None),
        P(AXES, None),
        P(AXES, None),
        P(),
        P(AXES, None),
        P(),
        P(AXES, None),
        P(AXES, None),
        P(None, EP, None),
        P(None, EP, None),
        P(None, EP, None),
    )
    return jax.shard_map(
        local, mesh=finer, in_specs=in_specs, out_specs=P(AXES, None), check_vma=False
    )
```

```python
import math

import jax
import jax.numpy as jnp
from jax import lax
from jax.experimental import pallas as pl
from jax.experimental.pallas import tpu as pltpu
from jax.sharding import Mesh
from jax.sharding import PartitionSpec as P


HEAD = 128
CAP = 40
SIZES = (4, 2, 4, 2, 2)
AXES = ("x", "yl", "z", "h", "c")
EP = ("z", "h", "c")


def flat(coords):
    place = 0
    for size, coord in zip(SIZES, coords):
        place = place * size + coord
    return place


def sent(value, rule):
    pairs = []
    for source in range(math.prod(SIZES)):
        rest, coords = source, []
        for size in reversed(SIZES):
            coords.append(rest % size)
            rest //= size
        cx, cyl, cz, ch, cc = reversed(coords)
        x, y, z, core = rule(cx, 2 * ch + cyl, cz, cc)
        pairs.append((source, flat((x % 4, y % 2, z % 4, y % 4 // 2, core))))
    return lax.ppermute(value, AXES, pairs)


def moved(value, x=0, y=0, z=0):
    return sent(value, lambda cx, cy, cz, cc: (cx + x, cy + y, cz + z, cc))


def crossed(value):
    return sent(value, lambda cx, cy, cz, cc: (cx, cy, cz, 1 - cc))


def mate(place, pairing):
    return place + (1 if (place + pairing) % 2 == 0 else -1)


def to_mate(value, along_x, along_z, switch):
    def rule(cx, cy, cz, cc):
        goal = 1 - cc if switch else cc
        return (mate(cx, goal) if along_x else cx, cy, mate(cz, goal) if along_z else cz, goal)

    return sent(value, rule)


def from_mate(value, along_x, along_z, switch):
    def rule(cx, cy, cz, cc):
        goal = 1 - cc if switch else cc
        return (mate(cx, cc) if along_x else cx, cy, mate(cz, cc) if along_z else cz, goal)

    return sent(value, rule)


def later(value, blocks, switch):
    count = math.prod(SIZES)
    return lax.ppermute(
        value, AXES, [(s, (s ^ switch) + blocks) for s in range(count - blocks)]
    )


def half_of(value, which):
    width = value.shape[-1] // 2
    return lax.dynamic_slice_in_dim(value, which * width, width, value.ndim - 1)


def by_core(first, own, other, axis):
    return jnp.where(
        first,
        jnp.concatenate([own, other], axis=axis),
        jnp.concatenate([other, own], axis=axis),
    )


def attend_kernel(core_ref, seen_ref, query_ref, *refs):
    key_refs, value_refs, (out_ref, key_table, value_table) = refs[:10], refs[10:20], refs[20:]
    core = core_ref[0]
    for place in range(10):
        slot = place - place % 2 + (1 - core if place % 2 else core)
        key_table[slot] = key_refs[place][...]
        value_table[slot] = value_refs[place][...]
    factor = math.log2(math.e) / math.sqrt(HEAD)
    tokens = 128
    row = lax.broadcasted_iota(jnp.int32, (tokens, tokens), 0)
    col = lax.broadcasted_iota(jnp.int32, (tokens, tokens), 1)
    causal = jnp.where(col <= row, 0.0, -1e30)
    keys = key_table[...].reshape(-1, HEAD)
    values = value_table[...].reshape(-1, HEAD)
    for block in range(2):
        here = slice(block * tokens, (block + 1) * tokens)
        key_window = keys[block * tokens : (block + 9) * tokens]
        value_window = values[block * tokens : (block + 9) * tokens]
        hidden = [
            jnp.full((tokens, tokens), jnp.where(seen_ref[block, 8 - place] > 0, 0.0, -1e30))
            for place in range(8)
        ]
        bias = jnp.concatenate(hidden + [causal], axis=1)
        query = jnp.concatenate(
            [query_ref[here, head * HEAD : (head + 1) * HEAD] for head in range(4)], axis=0
        )
        scores = lax.dot_general(
            query, key_window, (((1,), (1,)), ((), ())), preferred_element_type=jnp.float32
        )
        weights, totals = [], []
        for head in range(4):
            score = scores[head * tokens : (head + 1) * tokens] + bias
            peak = jnp.max(score, axis=1, keepdims=True)
            weight = jnp.exp2((score - peak) * factor)
            totals.append(jnp.sum(weight, axis=1, keepdims=True))
            weights.append(weight.astype(jnp.bfloat16))
        mixed = jnp.dot(
            jnp.concatenate(weights, axis=0), value_window, preferred_element_type=jnp.float32
        )
        for head in range(4):
            result = mixed[head * tokens : (head + 1) * tokens] / totals[head]
            lanes = slice(head // 2 * HEAD, head // 2 * HEAD + HEAD)
            out_ref[0, head % 2, here, lanes] = result.astype(jnp.bfloat16)


def attend(core, seen, query, windows):
    key_specs = [pl.BlockSpec((128, HEAD), lambda j: (0, j)) for _ in windows]
    value_specs = [pl.BlockSpec((128, HEAD), lambda j: (0, 4 + j)) for _ in windows]
    return pl.pallas_call(
        attend_kernel,
        grid=(4,),
        in_specs=[
            pl.BlockSpec(memory_space=pltpu.SMEM),
            pl.BlockSpec(memory_space=pltpu.SMEM),
            pl.BlockSpec((256, 4 * HEAD), lambda j: (0, j)),
            *key_specs,
            *value_specs,
        ],
        out_specs=pl.BlockSpec((1, 2, 256, 256), lambda j: (j // 2, 0, 0, j % 2)),
        out_shape=jax.ShapeDtypeStruct((2, 2, 256, 512), jnp.bfloat16),
        scratch_shapes=[
            pltpu.VMEM((10, 128, HEAD), jnp.bfloat16),
            pltpu.VMEM((10, 128, HEAD), jnp.bfloat16),
        ],
        name="attend",
        cost_estimate=pl.CostEstimate(
            flops=6_000_000_000, transcendentals=5_000_000, bytes_accessed=6_000_000
        ),
    )(core.reshape(1), seen, query, *windows, *windows)


def in_order(pieces, own_index):
    count = len(pieces)
    table = jnp.zeros((count, *pieces[0].shape), pieces[0].dtype)
    for step, piece in enumerate(pieces):
        table = lax.dynamic_update_index_in_dim(table, piece, (own_index - step) % count, 0)
    return table


def by_height(pieces, place_y):
    x_half, z_half, rows, columns = pieces[0][2].shape
    table = jnp.zeros((x_half, 2, z_half, 2, rows, columns), pieces[0][2].dtype)
    for step, column, piece in pieces:
        source = (place_y - step) % 4
        piece = piece.reshape(x_half, 1, z_half, 1, rows, -1)
        table = lax.dynamic_update_slice(table, piece, (0, source % 2, 0, source // 2, 0, column))
    return table


def project_kernel(core_ref, *refs):
    same, other, (rows_own, rows_other) = refs[:8], refs[8:16], refs[16:18]
    left = jnp.concatenate([ref[0] for ref in same], axis=0)
    right = jnp.concatenate([ref[0] for ref in other], axis=0)
    product = jnp.dot(left, rows_own[0], preferred_element_type=jnp.float32)
    product += jnp.dot(right, rows_other[0], preferred_element_type=jnp.float32)
    product = product.astype(jnp.bfloat16)
    for place, out_ref in enumerate(refs[18:]):
        out_ref[...] = product[place * 128 : (place + 1) * 128]


def project(core, same, other, rows):
    columns = 512
    same = [heads.reshape(2, 128, 512) for heads in same for _ in range(2)]
    other = [heads.reshape(2, 128, 512) for heads in other for _ in range(2)]
    here = pl.BlockSpec((1, 128, 512), lambda n, core: (core[0], 0, 0))
    there = pl.BlockSpec((1, 128, 512), lambda n, core: (1 - core[0], 0, 0))
    out = pl.BlockSpec((128, columns), lambda n, core: (0, n))
    shape = jax.ShapeDtypeStruct((128, rows.shape[2]), jnp.bfloat16)
    return pl.pallas_call(
        project_kernel,
        grid_spec=pltpu.PrefetchScalarGridSpec(
            num_scalar_prefetch=1,
            grid=(4,),
            in_specs=[
                *[here, there] * 8,
                pl.BlockSpec((1, 512, columns), lambda n, core: (core[0], 0, n)),
                pl.BlockSpec((1, 512, columns), lambda n, core: (1 - core[0], 0, n)),
            ],
            out_specs=[out] * 8,
        ),
        out_shape=[shape] * 8,
        name="project",
        cost_estimate=pl.CostEstimate(
            flops=4_300_000_000, transcendentals=0, bytes_accessed=10_000_000
        ),
    )(core.reshape(1), *same, *other, rows, rows)


def expert_kernel(*refs):
    slot_refs, (gate_ref, up_ref, down_ref, own_ref, other_ref) = refs[:4], refs[4:9]
    gate_sum, up_sum, act = refs[9:]
    step = pl.program_id(0)
    contract = (((1,), (1,)), ((), ()))

    @pl.when(step == 0)
    def _():
        gate_sum[...] = jnp.zeros_like(gate_sum)
        up_sum[...] = jnp.zeros_like(up_sum)

    @pl.when(step < 2)
    def _():
        slots = jnp.concatenate([ref[...] for ref in slot_refs], axis=0)
        gate = lax.dot_general(slots, gate_ref[0], contract, preferred_element_type=jnp.float32)
        up = lax.dot_general(slots, up_ref[0], contract, preferred_element_type=jnp.float32)
        gate_sum[...] += gate
        up_sum[...] += up

        @pl.when(step == 1)
        def _():
            value = gate_sum[...]
            act[...] = (value / (1.0 + jnp.exp(-value)) * up_sum[...]).astype(jnp.bfloat16)

    @pl.when(step >= 2)
    def _():
        part, half = 512, own_ref.shape[0]

        @pl.loop(0, own_ref.shape[1] // part)
        def _(place):
            lanes = pl.ds(pl.multiple_of(place * part, part), part)
            result = jnp.dot(
                act[...], down_ref[0, :, lanes], preferred_element_type=jnp.float32
            ).astype(jnp.bfloat16)
            own_ref[:, lanes] = result[:half]
            other_ref[:, lanes] = result[half:]


def expert(which, pieces, gate, up, down):
    slots, width = pieces[0].shape
    hidden = gate.shape[1]
    chunk = width // 2
    rows = len(pieces) * slots
    early = lambda step: jnp.minimum(step, 1)
    late = lambda step: jnp.maximum(step - 2, 0)
    out = pl.BlockSpec((rows // 2, chunk), lambda step: (0, late(step)))
    shape = jax.ShapeDtypeStruct((rows // 2, width), jnp.bfloat16)
    return pl.pallas_call(
        expert_kernel,
        grid=(4,),
        in_specs=[
            *[pl.BlockSpec((slots, chunk), lambda step: (0, early(step))) for _ in pieces],
            pl.BlockSpec((1, hidden, chunk), lambda step: (which, 0, early(step))),
            pl.BlockSpec((1, hidden, chunk), lambda step: (which, 0, early(step))),
            pl.BlockSpec((1, hidden, chunk), lambda step: (which, 0, late(step))),
        ],
        out_specs=[out, out],
        out_shape=[shape, shape],
        scratch_shapes=[
            pltpu.VMEM((rows, hidden), jnp.float32),
            pltpu.VMEM((rows, hidden), jnp.float32),
            pltpu.VMEM((rows, hidden), jnp.bfloat16),
        ],
        name="expert",
        cost_estimate=pl.CostEstimate(
            flops=7_000_000_000, transcendentals=300_000, bytes_accessed=22_000_000
        ),
    )(*pieces, gate, up, down)


def total(*terms):
    return sum(term.astype(jnp.float32) for term in terms).astype(jnp.bfloat16)


def gather_slots(own):
    flip = moved(own, y=2)
    far = moved(own, z=2)
    flip_far = moved(far, y=2)
    both = jnp.concatenate([own, flip], axis=0)
    ring1, ring3 = moved(both, z=1), moved(both, z=3)
    early = jnp.concatenate([both, far, flip_far], axis=0)
    early_got = crossed(early)
    late = jnp.concatenate([ring1, ring3], axis=0)
    late_got = crossed(late)
    return [early, late, early_got, late_got]


def return_sums(own_part, other_part):
    swapped = crossed(other_part)

    def owed(place, count=1):
        rows = slice(place * CAP, (place + count) * CAP)
        return total(own_part[rows], swapped[rows])

    here, flip, far, flip_far, ring1, ring3 = lax.optimization_barrier(
        (owed(0), owed(1), owed(2), owed(3), owed(4, 2), owed(6, 2))
    )
    flip_far = moved(flip_far, y=2)
    ring1, ring3 = moved(ring1, z=3), moved(ring3, z=1)
    across = moved(total(flip, ring1[CAP:], ring3[CAP:]), y=2)
    twice = moved(total(far, flip_far), z=2)
    return sum(t.astype(jnp.float32) for t in (here, ring1[:CAP], ring3[:CAP], across, twice))


def local(
    residual,
    queries,
    key_rows,
    value_rows,
    visible,
    out_proj,
    norm_gain,
    expert_ids,
    route_weight,
    expert_gate,
    expert_up,
    expert_down,
):
    core = lax.axis_index("c")
    first = core == 0
    tokens = residual.shape[0]
    place_x, place_z = lax.axis_index("x"), lax.axis_index("z")
    place_y = 2 * lax.axis_index("h") + lax.axis_index("yl")

    kv_own = jnp.concatenate([half_of(key_rows, core), half_of(value_rows, core)], axis=1)
    kv_give = jnp.concatenate([half_of(key_rows, 1 - core), half_of(value_rows, 1 - core)], axis=1)
    kv_got = crossed(kv_give)
    query_got = crossed(half_of(queries, 1 - core))
    query_two = by_core(first, half_of(queries, core), query_got, 0)
    windows = []
    for blocks in (8, 6, 4, 2):
        windows += [later(kv_own, blocks, 0), later(kv_give, blocks, 1)]
    windows += [kv_own, kv_got]

    columns = out_proj.shape[1] // 2
    rows_got = moved(out_proj, z=2)
    rows = in_order([out_proj, rows_got], place_z // 2)
    rows_got = crossed(half_of(rows, 1 - core))
    rows = by_core(first, half_of(rows, core), rows_got, 1)
    rows_got = moved(rows, x=2)
    rows = in_order([rows, rows_got], place_x // 2)
    rows_up, rows_down = moved(rows, y=1), moved(rows, y=3)
    half = columns // 2
    far_low, far_high = moved(rows_up[..., :half], y=1), moved(rows_down[..., half:], y=3)
    pieces = [(0, 0, rows), (1, 0, rows_up), (3, 0, rows_down), (2, 0, far_low), (2, half, far_high)]
    rows = by_height(pieces, place_y).reshape(2, -1, columns)

    chip_block = lax.axis_index(AXES) - core
    seen = lax.dynamic_slice_in_dim(visible, chip_block, 2, 0)
    attended = attend(core, seen, query_two, windows)
    attended = attended.reshape(4, 2 * tokens, -1)

    ways = ((1, 1), (1, 0), (0, 1), (0, 0))
    same, other = [], []
    for along_x, along_z in ways:
        wanted = (place_x % 2 ^ along_x) * 2 + (place_z % 2 ^ along_z)
        piece = lax.dynamic_index_in_dim(attended, wanted, 0, keepdims=False)
        remote = along_x or along_z
        same.append(to_mate(piece, along_x, along_z, False) if remote else piece)
        other.append(to_mate(piece, along_x, along_z, True) if remote else crossed(piece))
    products = project(core, same, other, rows)
    straight, switched = [], []
    for place, (along_x, along_z) in enumerate(ways):
        here, there = products[2 * place : 2 * place + 2]
        if along_x or along_z:
            here = from_mate(here, along_x, along_z, False)
            there = from_mate(there, along_x, along_z, True)
        else:
            there = crossed(there)
        straight.append(here.astype(jnp.float32))
        switched.append(there.astype(jnp.float32))
    projected = by_core(first, sum(straight), sum(switched), 1)

    hidden_sum = residual.astype(jnp.float32) + projected
    mean_square = jnp.mean(hidden_sum * hidden_sum, axis=-1, keepdims=True)
    normed = (hidden_sum * lax.rsqrt(mean_square + 1e-05) * norm_gain).astype(jnp.bfloat16)

    mixes, slots = [], []
    for which in range(expert_gate.shape[0]):
        choose = expert_ids == which
        member = jnp.any(choose, axis=1)
        token_weight = jnp.sum(jnp.where(choose, route_weight, 0.0), axis=1)
        ranked = jnp.cumsum(member.astype(jnp.int32)) - member.astype(jnp.int32)
        slot_hit = (ranked[None, :] == jnp.arange(CAP, dtype=jnp.int32)[:, None]) & member[None, :]
        slots.append(slot_hit.astype(jnp.bfloat16))
        mixes.append(jnp.where(slot_hit, token_weight[None, :], 0.0))
    outgoing = jnp.dot(
        jnp.concatenate(slots, axis=0), normed, preferred_element_type=jnp.float32
    ).astype(jnp.bfloat16)

    returned = []
    for which in range(expert_gate.shape[0]):
        pieces = gather_slots(outgoing[which * CAP : (which + 1) * CAP])
        parts = expert(which, pieces, expert_gate, expert_up, expert_down)
        returned.append(return_sums(*parts))
    expert_mix = jnp.dot(
        jnp.concatenate(mixes, axis=0).T,
        jnp.concatenate(returned, axis=0),
        precision=lax.Precision.HIGHEST,
    )
    return (hidden_sum + expert_mix).astype(jnp.bfloat16)


def solution(mesh):
    finer = Mesh(mesh.devices.reshape(SIZES), AXES)
    in_specs = (
        P(AXES, None),
        P(AXES, None),
        P(AXES, None),
        P(AXES, None),
        P(),
        P(AXES, None),
        P(),
        P(AXES, None),
        P(AXES, None),
        P(None, EP, None),
        P(None, EP, None),
        P(None, EP, None),
    )
    return jax.shard_map(
        local, mesh=finer, in_specs=in_specs, out_specs=P(AXES, None), check_vma=False
    )
```
